128 devices in a mesh: gx: 4 (over y), gy: 32 (over z, x, core).
Axes of the slice: x: 4, y: 4, z: 4, core: 2. Of those that a mesh axis runs over, the one named last changes fastest.
Arguments:
- point_coords: float32 [512, 3, 256], P(('gx', 'gy')), may hold values from -2 to 2
- charge: float32 [512, 256], P(('gx', 'gy')), may hold values from -0.12 to 0.12
- shell_index: int32 [512, 32, 256], P(('gx', 'gy')), may hold values from 0 to 63
- neighbours: int32 [512, 32], P(('gx', 'gy')), may hold values from 0 to 4095, as said below
- neighbour_count: int32 [512], P(('gx', 'gy')), may hold values from 24 to 32
- batch_load: int32 [128], P(('gx', 'gy')), may hold values from 3 to 4, as said below
- atom_coords: float32 [3, 4096], replicated, may hold values from -2 to 2
- owner_slot: int32 [4096], replicated, may hold values from 0 to 4095, as said below
Outputs:
- potential: float32 [512, 256], P(('gx', 'gy'))
- moments: float32 [4096, 3136], P(('gx', 'gy'))
The draws below stay inside these ranges and needn't reach their ends.
Inputs may be any that keep to these rules, and one draw needn't show every extreme that they name: `neighbours`: atom labels. On every device, at most 1 of its 128 neighbour slots, live or not, name atoms whose owner_slot lies in one block of 32 rows; on every device some block gets exactly 1. `owner_slot`: each row number once. `batch_load`: some device has all 4 slots live.
All inputs are finite; a program needn't handle non-finite values.
Results may differ from the reference program's by a relative error of at most 0.0003.
Values sent between devices are 32-bit elements; how exact they have to be, the bound alone decides.
A program may use at most 64 MiB of HBM per device.

```python
import math
import jax
import jax.numpy as jnp
from jax import lax

LM = 49
SHELLS = 64
PTS = 256
NB = 32
BSLOT = 4
ATOM_DEV = 32
NBATCH = 512
ATOMS = 4096
CAP = 1
DEVICES = 128


def owner_table(key):
    return jax.random.permutation(jax.random.fold_in(key, 7), ATOMS).astype(jnp.int32)


def draw_owner_slot(key, part):
    return owner_table(key)


def draw_neighbours(key, part):
    table = owner_table(key)
    inverse = jnp.zeros((ATOMS,), jnp.int32).at[table].set(jnp.arange(ATOMS, dtype=jnp.int32))
    row_total = BSLOT * NB
    spaces = DEVICES * CAP

    def one_device(device_key):
        first_key, score_key, local_key, shuffle_key = jax.random.split(device_key, 4)
        chosen = jax.random.randint(first_key, (), 0, DEVICES)
        spot = jnp.arange(spaces, dtype=jnp.int32)
        target = spot // CAP
        noise = jax.random.randint(score_key, (spaces,), 1, 2 ** 20)
        scores = jnp.where(target == chosen, spot, noise * spaces + spot)
        ranked = jnp.argsort(scores)
        destination = target[ranked[:row_total]]
        destination = jax.random.permutation(shuffle_key, destination)
        local = jax.random.randint(local_key, (row_total,), 0, ATOM_DEV)
        return inverse[destination * ATOM_DEV + local].reshape(BSLOT, NB)
    keys = jax.random.split(jax.random.fold_in(key, 11), DEVICES)
    return jax.vmap(one_device)(keys).reshape(DEVICES * BSLOT, NB).astype(jnp.int32)


def draw_batch_load(key, part):
    loads = jax.random.randint(jax.random.fold_in(key, 3), (DEVICES,), 3 * BSLOT // 4, BSLOT + 1)
    busiest = jax.random.randint(jax.random.fold_in(key, 5), (), 0, DEVICES)
    return jnp.where(jnp.arange(DEVICES) == busiest, BSLOT, loads).astype(jnp.int32)


def place_ends(entries, own_key, low, high):
    place = [jax.random.randint(jax.random.fold_in(own_key, axis), (), 0, length) for axis, length in enumerate(entries.shape)]
    main_axis = entries.shape.index(max(entries.shape))
    next_to = place[:main_axis] + [(place[main_axis] + 1) % entries.shape[main_axis]] + place[main_axis + 1:]
    return entries.at[tuple(place)].set(low).at[tuple(next_to)].set(high)


def levels(own_key, extent, cuts, smallest, largest):
    def one(axis_at, shards_of):
        heights = jax.random.uniform(jax.random.fold_in(jax.random.fold_in(own_key, 6), axis_at), (shards_of,), jnp.float32, smallest / len(cuts), largest / len(cuts))
        return jnp.repeat(jnp.exp(heights), extent[axis_at] // shards_of).reshape((-1,) + (1,) * (len(extent) - axis_at - 1))

    gain = one(*cuts[0])
    for cut in cuts[1:]:
        gain = gain * one(*cut)
    return gain


def scatter_about(own_key, extent, spread, bound, cuts=(), kind=jnp.bfloat16):
    values = spread * jax.random.normal(own_key, extent, jnp.float32)
    if cuts:
        values = values * levels(own_key, extent, cuts, -0.22, 0.18)
    return jnp.clip(values, -bound, bound).astype(kind)


def setup_inputs(seed: int = 0) -> dict:
    splits = jax.random.split(jax.random.key(seed), 9)
    return {
        "point_coords": jnp.clip(jax.random.uniform(splits[0], (NBATCH, 3, PTS), jnp.float32, -2.0, 2.0) * levels(splits[0], (NBATCH, 3, PTS), ((0, 128),), -0.4, 0.0), -2.0, 2.0),
        "charge": scatter_about(splits[1], (NBATCH, PTS), 0.02, 0.12, ((0, 128),), jnp.float32),
        "shell_index": place_ends(jax.random.randint(splits[2], (NBATCH, NB, PTS), 0, SHELLS), jax.random.fold_in(splits[2], 1), 0, SHELLS - 1).astype(jnp.int32),
        "neighbours": draw_neighbours(jax.random.fold_in(splits[8], 71), 0),
        "neighbour_count": place_ends(jax.random.randint(splits[4], (NBATCH,), 3 * NB // 4, NB + 1), jax.random.fold_in(splits[4], 1), 3 * NB // 4, NB).astype(jnp.int32),
        "batch_load": draw_batch_load(jax.random.fold_in(splits[8], 71), 0),
        "atom_coords": jnp.clip(jax.random.uniform(splits[6], (3, ATOMS), jnp.float32, -2.0, 2.0), -2.0, 2.0),
        "owner_slot": draw_owner_slot(jax.random.fold_in(splits[8], 71), 0),
    }


SOFTEN = 0.01

def harmonics(along_x, along_y, along_z):
    cosines = [jnp.ones_like(along_x)]
    sines = [jnp.zeros_like(along_x)]
    for azimuth in range(1, 7):
        previous_cos = cosines[-1]
        previous_sin = sines[-1]
        cosines.append(previous_cos * along_x - previous_sin * along_y)
        sines.append(previous_cos * along_y + previous_sin * along_x)
    legendre = {}
    for azimuth in range(7):
        legendre[azimuth, azimuth] = jnp.ones_like(along_z) * float(math.prod(range(1, 2 * azimuth, 2)))
        if azimuth < 6:
            legendre[azimuth + 1, azimuth] = (2 * azimuth + 1) * along_z * legendre[azimuth, azimuth]
        for degree in range(azimuth + 2, 7):
            legendre[degree, azimuth] = ((2 * degree - 1) * along_z * legendre[degree - 1, azimuth] - (degree + azimuth - 1) * legendre[degree - 2, azimuth]) / (degree - azimuth)
    results = []
    for degree in range(7):
        for signed in range(-degree, degree + 1):
            azimuth = abs(signed)
            factor = math.sqrt((2 * degree + 1) / (4 * math.pi) * math.factorial(degree - azimuth) / math.factorial(degree + azimuth))
            if signed == 0:
                results.append(factor * legendre[degree, 0])
            elif signed > 0:
                results.append(math.sqrt(2.0) * factor * legendre[degree, azimuth] * cosines[azimuth])
            else:
                results.append(math.sqrt(2.0) * factor * legendre[degree, azimuth] * sines[azimuth])
    return jnp.stack(results)

def green_table():
    shell_rank = jnp.arange(SHELLS, dtype=jnp.float32)
    radius = 0.5 * jnp.exp(2.3 * shell_rank / SHELLS)
    nearer = jnp.minimum(radius[:, None], radius[None, :])
    farther = jnp.maximum(radius[:, None], radius[None, :])
    kernels = []
    for degree in range(7):
        kernel = 4.0 * math.pi / (2 * degree + 1) * nearer ** degree / farther ** (degree + 1)
        kernels.extend([kernel] * (2 * degree + 1))
    return jnp.stack(kernels)

def batch_geometry(coords, atom_place, count):
    offset = coords[:, None, :] - atom_place[:, :, None]
    squared = lax.optimization_barrier(jnp.sum(offset * offset, axis=0))
    scale = 1.0 / jnp.sqrt(squared + SOFTEN)
    harmonic = harmonics(offset[0] * scale, offset[1] * scale, offset[2] * scale)
    slot_live = jnp.arange(atom_place.shape[1], dtype=jnp.int32) < count
    closeness = jnp.where(slot_live[:, None], 1.0 / (1.0 + squared), 0.0)
    share = closeness / lax.optimization_barrier(jnp.sum(closeness, axis=0, keepdims=True))
    return (harmonic, share, slot_live)

def reference(point_coords, charge, shell_index, neighbours, neighbour_count, batch_load, atom_coords, owner_slot):
    total_batches = charge.shape[0]
    batch_rank = jnp.arange(total_batches, dtype=jnp.int32)
    live_batch = (batch_rank % BSLOT < batch_load[batch_rank // BSLOT]).astype(jnp.float32)
    slot_rank = jnp.arange(NB, dtype=jnp.int32)

    def forward(moments, inputs):
        coords, weights_here, shells_here, labels, count, live = inputs
        harmonic, share, slot_live = batch_geometry(coords, atom_coords[:, labels], count)
        weighted = harmonic * (share * weights_here[None, :] * live)[None]
        segment = (slot_rank[:, None] * SHELLS + shells_here).reshape(-1).astype(jnp.int32)
        data = jnp.transpose(weighted, (1, 2, 0)).reshape(-1, harmonic.shape[0])
        summed = jax.ops.segment_sum(data, segment, num_segments=NB * SHELLS)
        partial_value = jnp.transpose(summed.reshape(NB, SHELLS, -1), (0, 2, 1))
        moments = moments.at[owner_slot[labels]].add(partial_value)
        return (moments, None)
    start = jnp.zeros((ATOMS, LM, SHELLS), jnp.float32)
    moments, _ = lax.scan(forward, start, (point_coords, charge, shell_index, neighbours, neighbour_count, live_batch))
    tables = jnp.einsum('lst,alt->als', green_table(), moments, precision=lax.Precision.HIGHEST)

    def evaluate(inputs):
        coords, shells_here, labels, count, live = inputs
        harmonic, share, slot_live = batch_geometry(coords, atom_coords[:, labels], count)
        table_rows = tables[owner_slot[labels]]
        spots = jnp.broadcast_to(shells_here[:, None, :], (NB, table_rows.shape[1], shells_here.shape[1]))
        picked = jnp.take_along_axis(table_rows, spots, axis=2)
        total = lax.optimization_barrier(jnp.sum(picked * jnp.transpose(harmonic, (1, 0, 2)), axis=1))
        return lax.optimization_barrier(jnp.sum(jnp.where(slot_live[:, None], total, 0.0), axis=0)) * live
    potential = lax.map(evaluate, (point_coords, shell_index, neighbours, neighbour_count, live_batch))
    return (potential, moments.reshape(ATOMS, LM * SHELLS))
```

```python
import functools
import math

import jax
import jax.numpy as jnp
import numpy as np
from jax import lax
from jax.experimental import pallas as pl
from jax.experimental.pallas import tpu as pltpu
from jax.sharding import PartitionSpec as P

MESH = pl.DeviceIdType.MESH
F32 = jnp.float32
BF16 = jnp.bfloat16
SHELLS = 64
LMAX = 6
LM = 49
KP = 56
SOFTEN = 0.01
ROWS = 11
PITCH = 16
SLOTP = 136


def green_pair():
    rank = np.arange(SHELLS, dtype=np.float64)
    radius = 0.5 * np.exp(2.3 * rank / SHELLS)
    nearer = np.minimum(radius[:, None], radius[None, :])
    farther = np.maximum(radius[:, None], radius[None, :])
    full = np.stack(
        [
            4.0 * math.pi / (2 * d + 1) * nearer**d / farther ** (d + 1)
            for d in range(LMAX + 1)
        ]
    )
    full = np.concatenate([full, full], axis=2).astype(np.float32)
    high = full.astype(jnp.bfloat16)
    low = (full - high.astype(np.float32)).astype(jnp.bfloat16)
    return high, low


def split(x):
    high = x.astype(BF16).astype(F32)
    return high, x - high


def dot(a, b, dims=((1,), (0,))):
    return lax.dot_general(a, b, (dims, ((), ())), preferred_element_type=F32)


def harmonics(ux, uy, uz):
    cosine = [None]
    sine = [None]
    for m in range(1, LMAX + 1):
        if m == 1:
            cosine.append(ux)
            sine.append(uy)
        else:
            pc, ps = cosine[-1], sine[-1]
            cosine.append(pc * ux - ps * uy)
            sine.append(pc * uy + ps * ux)

    def norm(d, m):
        value = math.sqrt(
            (2 * d + 1) / (4 * math.pi) * math.factorial(d - m) / math.factorial(d + m)
        )
        return value * (math.sqrt(2.0) if m else 1.0)

    out = {}
    for m in range(LMAX + 1):
        start = norm(m, m) * float(math.prod(range(1, 2 * m, 2)))
        older, old = None, None
        for d in range(m, LMAX + 1):
            if d == m:
                now = start
            elif d == m + 1:
                now = uz * ((2 * m + 1) * start * norm(d, m) / norm(m, m))
            else:
                ca = (2 * d - 1) / (d - m) * norm(d, m) / norm(d - 1, m)
                cb = (d + m - 1) / (d - m) * norm(d, m) / norm(d - 2, m)
                now = (ca * uz) * old - cb * older
            if m == 0:
                out[d * d + d] = now if d else jnp.full(ux.shape, start, F32)
            else:
                out[d * d + d + m] = cosine[m] * now
                out[d * d + d - m] = sine[m] * now
            older, old = old, now
    return out


def pack_kernel(
    labels, count, load, owner, atoms, coords, charge, shell, pay, meta, place, src
):
    batches, slots = labels.shape
    spaces = batches * slots
    devices = pay.shape[0]
    owned = owner.shape[0] // devices

    for b in range(batches):

        @pl.loop(0, slots, unroll=4)
        def _(s):
            label = labels[b, s]
            target = owner[label]
            row = b * slots + s
            for c in range(3):
                place[c, pl.ds(row, 1), :] = jnp.full((1, 128), atoms[c, label], F32)
            place[3, pl.ds(row, 1), :] = jnp.full(
                (1, 128), (target // owned).astype(F32), F32
            )
            src[10, pl.ds(row, 1), :] = jnp.full(
                (1, 128), (target % owned).astype(F32), F32
            )

    slot_rank = lax.broadcasted_iota(jnp.int32, (slots, 128), 0)
    lane = lax.broadcasted_iota(jnp.int32, (slots, 128), 1)
    lives = []
    for b in range(batches):
        live = jnp.where(b < load[0], 1.0, 0.0).astype(F32)
        slot_live = slot_rank < count[b]
        here = slice(b * slots, (b + 1) * slots)
        lives.append(jnp.where(slot_live & (lane == b), live, 0.0))
        for h in range(2):
            points = slice(h * 128, (h + 1) * 128)
            squared = 0.0
            for c in range(3):
                offset = coords[b, c : c + 1, points] - place[c, here, :]
                src[2 * c + h, here, :] = offset
                squared = squared + offset * offset
            closeness = jnp.where(slot_live, 1.0 / (1.0 + squared), 0.0)
            total = jnp.sum(closeness, axis=0, keepdims=True)
            scaled = charge[b : b + 1, points] * live / total
            src[6 + h, here, :] = shell[b, :, points].astype(F32)
            src[8 + h, here, :] = jnp.where(slot_live, scaled, 0.0)

    goes = (
        place[3] == lax.broadcasted_iota(jnp.int32, (spaces, devices), 1).astype(F32)
    ).astype(F32)
    goes = goes.T.astype(BF16)
    flat = pay.reshape(devices * PITCH, 128)
    for r in range(ROWS):
        block = src[r]
        high, rest = split(block)
        if r in (6, 7, 10):
            moved = dot(goes, high.astype(BF16))
        else:
            middle, low = split(rest)
            moved = (
                dot(goes, high.astype(BF16))
                + dot(goes, middle.astype(BF16))
                + dot(goes, low.astype(BF16))
            )
        flat[pl.ds(r, devices, stride=PITCH), :] = moved
    meta[...] = dot(goes, jnp.concatenate(lives, axis=0).astype(BF16))


def place_of():
    gx, gy = lax.axis_size("gx"), lax.axis_size("gy")
    me = lax.axis_index("gx") * gy + lax.axis_index("gy")
    return me, gx * gy, gy


def barrier_all(me, devices, gy):
    barrier = pltpu.get_barrier_semaphore()

    @pl.loop(1, devices)
    def _(i):
        peer = lax.rem(me + i, devices)
        pl.semaphore_signal(
            barrier, inc=1, device_id=(peer // gy, lax.rem(peer, gy)), device_id_type=MESH
        )

    pl.semaphore_wait(barrier, devices - 1)


def send_all(me, devices, gy, source, target, send_sem, recv_sem):
    @pl.loop(1, devices)
    def _(i):
        peer = lax.rem(me + i, devices)
        pltpu.make_async_remote_copy(
            src_ref=source(peer),
            dst_ref=target(me),
            send_sem=send_sem,
            recv_sem=recv_sem,
            device_id=(peer // gy, lax.rem(peer, gy)),
            device_id_type=MESH,
        ).start()


def exchange_kernel(rows, pay, arrived, send_sem, recv_sem):
    me, devices, gy = place_of()
    barrier_all(me, devices, gy)
    send_all(
        me,
        devices,
        gy,
        lambda i: pay.at[i, pl.ds(0, rows)],
        lambda i: arrived.at[i, pl.ds(0, rows)],
        send_sem,
        recv_sem,
    )
    arrived[me] = pay[me]
    every = pltpu.make_async_remote_copy(
        src_ref=pay.at[pl.ds(0, devices - 1), pl.ds(0, rows)],
        dst_ref=arrived.at[pl.ds(0, devices - 1), pl.ds(0, rows)],
        send_sem=send_sem,
        recv_sem=recv_sem,
        device_id=(0, 0),
        device_id_type=MESH,
    )
    every.wait_send()
    every.wait_recv()


def owner_kernel(arrived, ghigh, glow, moments, reply, ys, ws, hots, parts, acc, tables):
    sources = arrived.shape[0]
    owned = moments.shape[0]
    flat = arrived.reshape(sources * PITCH, 128)
    groups = sources // 8

    @pl.loop(0, groups)
    def _(g):
        for h in range(2):

            def row(r):
                return flat[pl.ds(g * 8 * PITCH + 2 * r + h, 8, stride=PITCH), :]

            dx, dy, dz = row(0), row(1), row(2)
            squared = dx * dx + dy * dy + dz * dz
            scale = lax.rsqrt(squared + SOFTEN)
            ws[h, pl.ds(pl.multiple_of(g * 8, 8), 8), :] = row(4) / (1.0 + squared)
            values = harmonics(dx * scale, dy * scale, dz * scale)
            for k in range(KP):
                value = values[k] if k < LM else jnp.zeros_like(dx)
                ys[h, pl.ds(g * 8 * KP + k, 8, stride=KP), :] = value

    shell_rank = lax.broadcasted_iota(jnp.int32, (SHELLS, 128), 0).astype(F32)

    def forward(i):
        stack, hot = [], []
        for h in range(2):
            y = ys[h, pl.ds(pl.multiple_of(i * KP, 8), KP), :]
            weighted = y * ws[h, pl.ds(i, 1), :]
            high, low = split(weighted)
            stack.append(jnp.concatenate([high, low], axis=0).astype(BF16))
            shells = flat[pl.ds(i * PITCH + 6 + h, 1), :]
            hot.append((shells == shell_rank).astype(F32).astype(BF16))
        hot = jnp.concatenate(hot, axis=1)
        hots[i] = hot
        both = dot(jnp.concatenate(stack, axis=1), hot, ((1,), (1,)))
        parts[pl.ds(i, KP, stride=SLOTP), :SHELLS] = both[:KP] + both[KP:]

    @pl.loop(0, sources // 4)
    def _(q):
        for e in range(4):
            forward(q * 4 + e)

    marks = flat[pl.ds(10, sources, stride=PITCH), :]
    picks = (
        marks == lax.broadcasted_iota(jnp.int32, (sources, 128), 1).astype(F32)
    ).astype(F32)
    gather = picks[:, :owned].astype(BF16)
    combine = picks.T[:owned].astype(BF16)
    combine = jnp.concatenate([combine, combine], axis=1)

    def summed(k):
        part = parts[pl.ds(k * SLOTP, sources), :SHELLS]
        high, low = split(part)
        both = jnp.concatenate([high, low], axis=0).astype(BF16)
        return dot(combine, both)

    for k in range(0, LM, 2):
        first = summed(k)
        acc[k * owned : (k + 1) * owned, :SHELLS] = first
        if k + 1 < LM:
            second = summed(k + 1)
            acc[(k + 1) * owned : (k + 2) * owned, :SHELLS] = second
            moments[:, k * SHELLS : (k + 2) * SHELLS] = jnp.concatenate(
                [first, second], axis=1
            )
        else:
            moments[:, k * SHELLS : (k + 1) * SHELLS] = first

    for d in range(LMAX + 1):
        begin, end = d * d, (d + 1) * (d + 1)
        high, low = split(acc[begin * owned : end * owned, :SHELLS])
        high, low = high.astype(BF16), low.astype(BF16)
        table = dot(high, ghigh[d]) + dot(low, ghigh[d]) + dot(high, glow[d])
        thigh, tlow = split(table)
        lane = lax.broadcasted_iota(jnp.int32, table.shape, 1)
        table = jnp.where(lane < SHELLS, thigh, tlow).astype(BF16)
        for k in range(begin, end):
            tables[k * SLOTP : k * SLOTP + sources, :] = dot(
                gather, table[(k - begin) * owned : (k - begin + 1) * owned]
            )
    for k in range(LM, KP):
        tables[k * SLOTP : k * SLOTP + sources, :] = jnp.zeros((sources, 128), F32)

    def evaluate(i):
        table = tables[pl.ds(i, KP, stride=SLOTP), :].astype(BF16)
        hot = hots[i]
        picked = dot(table, jnp.concatenate([hot, hot], axis=0))
        for h in range(2):
            y = ys[h, pl.ds(pl.multiple_of(i * KP, 8), KP), :]
            total = jnp.sum(
                picked[:, h * 128 : (h + 1) * 128] * y, axis=0, keepdims=True
            )
            reply[pl.ds(i, 1), h, :] = total

    @pl.loop(0, sources // 4)
    def _(q):
        for e in range(4):
            evaluate(q * 4 + e)


def return_kernel(reply, meta, potential, back, send_sem, recv_sem):
    me, devices, gy = place_of()
    barrier_all(me, devices, gy)
    send_all(
        me,
        devices,
        gy,
        lambda i: reply.at[i],
        lambda i: back.at[i],
        send_sem,
        recv_sem,
    )
    back[me] = reply[me]
    every = pltpu.make_async_remote_copy(
        src_ref=reply.at[pl.ds(0, devices - 1)],
        dst_ref=back.at[pl.ds(0, devices - 1)],
        send_sem=send_sem,
        recv_sem=recv_sem,
        device_id=(0, 0),
        device_id_type=MESH,
    )
    every.wait_send()
    every.wait_recv()
    batches = potential.shape[0]
    mine = meta[...].T[: max(batches, 8)].astype(BF16)
    for h in range(2):
        high, rest = split(back[:, h, :])
        middle, low = split(rest)
        total = (
            dot(mine, high.astype(BF16))
            + dot(mine, middle.astype(BF16))
            + dot(mine, low.astype(BF16))
        )
        potential[:, h * 128 : (h + 1) * 128] = total[:batches]


VMEM = pl.BlockSpec(memory_space=pltpu.VMEM)
SMEM = pl.BlockSpec(memory_space=pltpu.SMEM)


def body(
    point_coords,
    charge,
    shell_index,
    neighbours,
    neighbour_count,
    batch_load,
    atom_coords,
    owner_slot,
):
    batches = charge.shape[0]
    slots = neighbours.shape[1]
    devices = lax.axis_size("gx") * lax.axis_size("gy")
    owned = owner_slot.shape[0] // devices
    spaces = batches * slots
    sds = jax.ShapeDtypeStruct
    pay, meta = pl.pallas_call(
        pack_kernel,
        out_shape=(sds((devices, PITCH, 128), F32), sds((devices, 128), F32)),
        in_specs=[SMEM] * 5 + [VMEM] * 3,
        out_specs=(VMEM, VMEM),
        scratch_shapes=[
            pltpu.VMEM((4, spaces, 128), F32),
            pltpu.VMEM((ROWS, spaces, 128), F32),
        ],
        name="pack",
    )(
        neighbours,
        neighbour_count,
        batch_load,
        owner_slot,
        atom_coords,
        point_coords,
        charge,
        shell_index,
    )
    arrived = pl.pallas_call(
        functools.partial(exchange_kernel, ROWS),
        out_shape=sds((devices, PITCH, 128), F32),
        in_specs=[VMEM],
        out_specs=VMEM,
        scratch_shapes=[pltpu.SemaphoreType.DMA, pltpu.SemaphoreType.DMA],
        compiler_params=pltpu.CompilerParams(collective_id=0, has_side_effects=True),
        name="exchange",
    )(pay)
    ghigh, glow = green_pair()
    moments, reply = pl.pallas_call(
        owner_kernel,
        out_shape=(sds((owned, LM * SHELLS), F32), sds((devices, 2, 128), F32)),
        in_specs=[VMEM] * 3,
        out_specs=(VMEM, VMEM),
        scratch_shapes=[
            pltpu.VMEM((2, devices * KP, 128), F32),
            pltpu.VMEM((2, devices, 128), F32),
            pltpu.VMEM((devices, SHELLS, 256), BF16),
            pltpu.VMEM((KP * SLOTP, 128), F32),
            pltpu.VMEM((LM * owned, 128), F32),
            pltpu.VMEM((KP * SLOTP, 128), F32),
        ],
        name="owner",
    )(arrived, jnp.asarray(ghigh), jnp.asarray(glow))
    potential = pl.pallas_call(
        return_kernel,
        out_shape=sds(charge.shape, F32),
        in_specs=[VMEM, VMEM],
        out_specs=VMEM,
        scratch_shapes=[
            pltpu.VMEM((devices, 2, 128), F32),
            pltpu.SemaphoreType.DMA,
            pltpu.SemaphoreType.DMA,
        ],
        compiler_params=pltpu.CompilerParams(collective_id=1, has_side_effects=True),
        name="giveback",
    )(reply, meta)
    return (potential, moments)


def solution(mesh):
    return jax.shard_map(
        body,
        mesh=mesh,
        in_specs=(
            P(("gx", "gy"), None, None),
            P(("gx", "gy"), None),
            P(("gx", "gy"), None, None),
            P(("gx", "gy"), None),
            P(("gx", "gy")),
            P(("gx", "gy")),
            P(),
            P(),
        ),
        out_specs=(P(("gx", "gy"), None), P(("gx", "gy"), None)),
        check_vma=False,
    )
```

```python
import math

import jax
import jax.numpy as jnp
import numpy as np
from jax import lax
from jax.experimental import pallas as pl
from jax.experimental.pallas import tpu as pltpu
from jax.sharding import PartitionSpec as P

MESH = pl.DeviceIdType.MESH
F32 = jnp.float32
BF16 = jnp.bfloat16
SHELLS = 64
LMAX = 6
LM = 49
KP = 56
SOFTEN = 0.01
ROWS = 11
PITCH = 16
SLOTP = 136
GROUPS = 8
WAVE = 16


def green_pair():
    rank = np.arange(SHELLS, dtype=np.float64)
    radius = 0.5 * np.exp(2.3 * rank / SHELLS)
    nearer = np.minimum(radius[:, None], radius[None, :])
    farther = np.maximum(radius[:, None], radius[None, :])
    full = np.stack(
        [
            4.0 * math.pi / (2 * d + 1) * nearer**d / farther ** (d + 1)
            for d in range(LMAX + 1)
        ]
    )
    full = np.concatenate([full, full], axis=2).astype(np.float32)
    high = full.astype(jnp.bfloat16)
    low = (full - high.astype(np.float32)).astype(jnp.bfloat16)
    return high, low


def split(x):
    high = x.astype(BF16).astype(F32)
    return high, x - high


def dot(a, b, dims=((1,), (0,))):
    return lax.dot_general(a, b, (dims, ((), ())), preferred_element_type=F32)


def harmonics(ux, uy, uz):
    cosine = [None]
    sine = [None]
    for m in range(1, LMAX + 1):
        if m == 1:
            cosine.append(ux)
            sine.append(uy)
        else:
            pc, ps = cosine[-1], sine[-1]
            cosine.append(pc * ux - ps * uy)
            sine.append(pc * uy + ps * ux)

    def norm(d, m):
        value = math.sqrt(
            (2 * d + 1) / (4 * math.pi) * math.factorial(d - m) / math.factorial(d + m)
        )
        return value * (math.sqrt(2.0) if m else 1.0)

    out = {}
    for m in range(LMAX + 1):
        start = norm(m, m) * float(math.prod(range(1, 2 * m, 2)))
        older, old = None, None
        for d in range(m, LMAX + 1):
            if d == m:
                now = start
            elif d == m + 1:
                now = uz * ((2 * m + 1) * start * norm(d, m) / norm(m, m))
            else:
                ca = (2 * d - 1) / (d - m) * norm(d, m) / norm(d - 1, m)
                cb = (d + m - 1) / (d - m) * norm(d, m) / norm(d - 2, m)
                now = (ca * uz) * old - cb * older
            if m == 0:
                out[d * d + d] = now if d else jnp.full(ux.shape, start, F32)
            else:
                out[d * d + d + m] = cosine[m] * now
                out[d * d + d - m] = sine[m] * now
            older, old = old, now
    return out


def decode(i):
    def ring(q):
        return q + (q // 2) * (5 - 2 * q)

    return ring(i // 32), ring(i // 8 % 4), ring(i // 2 % 4), i % 2


def peer_of(i, sign, y, z, x, c):
    dy, dz, dx, dc = decode(i)
    return (
        lax.rem(y + sign * dy + 4, 4),
        lax.rem(z + sign * dz + 4, 4) * 8
        + lax.rem(x + sign * dx + 4, 4) * 2
        + lax.rem(c + dc, 2),
    )


def fused_kernel(
    labels,
    count,
    load,
    owner,
    atoms,
    coords,
    charge,
    shell,
    ghigh,
    glow,
    moments,
    potential,
    place,
    src,
    pay,
    arrived,
    ys,
    ws,
    hots,
    parts,
    acc,
    tables,
    reply,
    back,
    send_sem,
    recv_sem,
    reply_send,
    reply_recv,
):
    batches, slots = labels.shape
    spaces = batches * slots
    devices = pay.shape[0]
    owned = moments.shape[0]
    gy = lax.axis_index("gy")
    here_at = (lax.axis_index("gx"), gy // 8, lax.rem(gy, 8) // 2, lax.rem(gy, 2))

    barrier = pltpu.get_barrier_semaphore()

    @pl.loop(1, devices)
    def _(i):
        pl.semaphore_signal(
            barrier, inc=1, device_id=peer_of(i, 1, *here_at), device_id_type=MESH
        )

    for b in range(batches):

        @pl.loop(0, slots, unroll=4)
        def _(s):
            label = labels[b, s]
            target = owner[label]
            row = b * slots + s
            for c in range(3):
                place[c, pl.ds(row, 1), :] = jnp.full((1, 128), atoms[c, label], F32)
            place[3, pl.ds(row, 1), :] = jnp.full(
                (1, 128), (target // owned).astype(F32), F32
            )
            src[10, pl.ds(row, 1), :] = jnp.full(
                (1, 128), lax.rem(target, owned).astype(F32), F32
            )

    slot_rank = lax.broadcasted_iota(jnp.int32, (slots, 128), 0)
    lane = lax.broadcasted_iota(jnp.int32, (slots, 128), 1)
    lives = []
    for b in range(batches):
        live = jnp.clip(load[0] - b, 0, 1).astype(F32)
        slot_live = jnp.clip(count[b] - slot_rank, 0, 1).astype(F32)
        here = slice(b * slots, (b + 1) * slots)
        lives.append(jnp.where(lane == b, slot_live * live, 0.0))
        for h in range(2):
            points = slice(h * 128, (h + 1) * 128)
            squared = 0.0
            for c in range(3):
                offset = coords[c, b : b + 1, points] - place[c, here, :]
                src[2 * c + h, here, :] = offset
                squared = squared + offset * offset
            closeness = slot_live / (1.0 + squared)
            total = jnp.sum(closeness, axis=0, keepdims=True)
            scaled = charge[b : b + 1, points] * live / total
            src[6 + h, here, :] = shell[b, :, points].astype(F32)
            src[8 + h, here, :] = slot_live * scaled

    py, pg = peer_of(
        lax.broadcasted_iota(jnp.int32, (spaces, devices), 1), 1, *here_at
    )
    goes = (place[3] == (py * 32 + pg).astype(F32)).astype(F32)
    goes = goes.T.astype(BF16)
    flat_pay = pay.reshape(devices * PITCH, 128)
    for r in range(ROWS):
        high, rest = split(src[r])
        moved = dot(goes, high.astype(BF16))
        if r not in (6, 7, 10):
            middle, low = split(rest)
            moved = (
                moved + dot(goes, middle.astype(BF16)) + dot(goes, low.astype(BF16))
            )
        flat_pay[pl.ds(r, devices, stride=PITCH), :] = moved
    mine = dot(goes, jnp.concatenate(lives, axis=0).astype(BF16))
    mine = mine.T[:8].astype(BF16)

    pl.semaphore_wait(barrier, devices - 1)

    def piece(ref, i, size=1):
        return ref.at[pl.ds(i, size), pl.ds(0, ROWS)]

    for g in range(GROUPS):

        @pl.loop(max(g * WAVE, 1), (g + 1) * WAVE)
        def _(i):
            pltpu.make_async_remote_copy(
                src_ref=piece(pay, i),
                dst_ref=piece(arrived, i),
                send_sem=send_sem,
                recv_sem=recv_sem.at[g],
                device_id=peer_of(i, 1, *here_at),
                device_id_type=MESH,
            ).start()

    arrived[0] = pay[0]
    flat = arrived.reshape(devices * PITCH, 128)
    shell_rank = lax.broadcasted_iota(jnp.int32, (SHELLS, 128), 0).astype(F32)

    def shapes(g):
        for h in range(2):

            def row(r):
                return flat[pl.ds(g * 8 * PITCH + 2 * r + h, 8, stride=PITCH), :]

            dx, dy, dz = row(0), row(1), row(2)
            squared = dx * dx + dy * dy + dz * dz
            scale = lax.rsqrt(squared + SOFTEN)
            ws[h, pl.ds(pl.multiple_of(g * 8, 8), 8), :] = row(4) / (1.0 + squared)
            values = harmonics(dx * scale, dy * scale, dz * scale)
            for k in range(KP):
                value = values[k] if k < LM else jnp.zeros_like(dx)
                ys[h, pl.ds(g * 8 * KP + k, 8, stride=KP), :] = value

    def forward(i):
        stack, hot = [], []
        for h in range(2):
            y = ys[h, pl.ds(pl.multiple_of(i * KP, 8), KP), :]
            weighted = y * ws[h, pl.ds(i, 1), :]
            high, low = split(weighted)
            stack.append(jnp.concatenate([high, low], axis=0).astype(BF16))
            shells = flat[pl.ds(i * PITCH + 6 + h, 1), :]
            hot.append((shells == shell_rank).astype(F32).astype(BF16))
        hot = jnp.concatenate(hot, axis=1)
        hots[i] = hot
        both = dot(jnp.concatenate(stack, axis=1), hot, ((1,), (1,)))
        parts[pl.ds(i, KP, stride=SLOTP), :SHELLS] = both[:KP] + both[KP:]

    for g in range(GROUPS):
        first = max(g * WAVE, 1)
        size = (g + 1) * WAVE - first
        pltpu.make_async_remote_copy(
            src_ref=piece(pay, first, size),
            dst_ref=piece(arrived, first, size),
            send_sem=send_sem,
            recv_sem=recv_sem.at[g],
            device_id=(0, 0),
            device_id_type=MESH,
        ).wait_recv()

        @pl.loop(0, WAVE // 8)
        def _(q):
            shapes(g * (WAVE // 8) + q)

        @pl.loop(0, WAVE // 4)
        def _(q):
            for e in range(4):
                forward(g * WAVE + q * 4 + e)

    marks = flat[pl.ds(10, devices, stride=PITCH), :]
    picks = (
        marks == lax.broadcasted_iota(jnp.int32, (devices, 128), 1).astype(F32)
    ).astype(F32)
    gather = picks[:, :owned].astype(BF16)
    combine = picks.T[:owned].astype(BF16)
    combine = jnp.concatenate([combine, combine], axis=1)
    for k in range(LM):
        high, low = split(parts[pl.ds(k * SLOTP, devices), :SHELLS])
        both = jnp.concatenate([high, low], axis=0).astype(BF16)
        acc[k * owned : (k + 1) * owned, :SHELLS] = dot(combine, both)

    for d in range(LMAX + 1):
        begin, end = d * d, (d + 1) * (d + 1)
        high, low = split(acc[begin * owned : end * owned, :SHELLS])
        high, low = high.astype(BF16), low.astype(BF16)
        table = dot(high, ghigh[d]) + dot(low, ghigh[d]) + dot(high, glow[d])
        thigh, tlow = split(table)
        lane_rank = lax.broadcasted_iota(jnp.int32, table.shape, 1)
        table = jnp.where(lane_rank < SHELLS, thigh, tlow).astype(BF16)
        for k in range(begin, end):
            tables[k * SLOTP : k * SLOTP + devices, :] = dot(
                gather, table[(k - begin) * owned : (k - begin + 1) * owned]
            )
    for k in range(LM, KP):
        tables[k * SLOTP : k * SLOTP + devices, :] = jnp.zeros((devices, 128), F32)

    def evaluate(i):
        table = tables[pl.ds(i, KP, stride=SLOTP), :].astype(BF16)
        hot = hots[i]
        picked = dot(table, jnp.concatenate([hot, hot], axis=0))
        for h in range(2):
            y = ys[h, pl.ds(pl.multiple_of(i * KP, 8), KP), :]
            total = jnp.sum(
                picked[:, h * 128 : (h + 1) * 128] * y, axis=0, keepdims=True
            )
            reply[pl.ds(i, 1), h, :] = total

    def answer(g):
        @pl.loop(max(g * WAVE, 1), (g + 1) * WAVE)
        def _(i):
            pltpu.make_async_remote_copy(
                src_ref=reply.at[pl.ds(i, 1)],
                dst_ref=back.at[pl.ds(i, 1)],
                send_sem=reply_send,
                recv_sem=reply_recv,
                device_id=peer_of(i, -1, *here_at),
                device_id_type=MESH,
            ).start()

    for g in reversed(range(GROUPS)):

        @pl.loop(0, WAVE // 4)
        def _(q):
            for e in range(4):
                evaluate(g * WAVE + q * 4 + e)

        if g + 1 < GROUPS:
            answer(g + 1)
    for k in range(0, LM, 2):
        first = acc[k * owned : (k + 1) * owned, :SHELLS]
        if k + 1 < LM:
            second = acc[(k + 1) * owned : (k + 2) * owned, :SHELLS]
            first = jnp.concatenate([first, second], axis=1)
        moments[:, k * SHELLS : min(k + 2, LM) * SHELLS] = first
    answer(0)
    back[0] = reply[0]

    everything = pltpu.make_async_remote_copy(
        src_ref=piece(pay, 1, devices - 1),
        dst_ref=piece(arrived, 1, devices - 1),
        send_sem=send_sem,
        recv_sem=recv_sem.at[0],
        device_id=(0, 0),
        device_id_type=MESH,
    )
    everything.wait_send()
    answers = pltpu.make_async_remote_copy(
        src_ref=reply.at[pl.ds(1, devices - 1)],
        dst_ref=back.at[pl.ds(1, devices - 1)],
        send_sem=reply_send,
        recv_sem=reply_recv,
        device_id=(0, 0),
        device_id_type=MESH,
    )
    answers.wait_send()
    answers.wait_recv()
    for h in range(2):
        high, rest = split(back[:, h, :])
        middle, low = split(rest)
        total = (
            dot(mine, high.astype(BF16))
            + dot(mine, middle.astype(BF16))
            + dot(mine, low.astype(BF16))
        )
        potential[:, h * 128 : (h + 1) * 128] = total[:batches]


VMEM = pl.BlockSpec(memory_space=pltpu.VMEM)
SMEM = pl.BlockSpec(memory_space=pltpu.SMEM)


def body(
    point_coords,
    charge,
    shell_index,
    neighbours,
    neighbour_count,
    batch_load,
    atom_coords,
    owner_slot,
):
    batches = charge.shape[0]
    slots = neighbours.shape[1]
    devices = lax.axis_size("gx") * lax.axis_size("gy")
    owned = owner_slot.shape[0] // devices
    spaces = batches * slots
    sds = jax.ShapeDtypeStruct
    ghigh, glow = green_pair()
    moments, potential = pl.pallas_call(
        fused_kernel,
        out_shape=(sds((owned, LM * SHELLS), F32), sds(charge.shape, F32)),
        in_specs=[SMEM] * 5 + [VMEM] * 5,
        out_specs=(VMEM, VMEM),
        scratch_shapes=[
            pltpu.VMEM((4, spaces, 128), F32),
            pltpu.VMEM((ROWS, spaces, 128), F32),
            pltpu.VMEM((devices, PITCH, 128), F32),
            pltpu.VMEM((devices, PITCH, 128), F32),
            pltpu.VMEM((2, devices * KP, 128), F32),
            pltpu.VMEM((2, devices, 128), F32),
            pltpu.VMEM((devices, SHELLS, 256), BF16),
            pltpu.VMEM((KP * SLOTP, 128), F32),
            pltpu.VMEM((LM * owned, 128), F32),
            pltpu.VMEM((KP * SLOTP, 128), F32),
            pltpu.VMEM((devices, 2, 128), F32),
            pltpu.VMEM((devices, 2, 128), F32),
            pltpu.SemaphoreType.DMA,
            pltpu.SemaphoreType.DMA((GROUPS,)),
            pltpu.SemaphoreType.DMA,
            pltpu.SemaphoreType.DMA,
        ],
        compiler_params=pltpu.CompilerParams(collective_id=0, has_side_effects=True),
        name="fused",
    )(
        neighbours,
        neighbour_count,
        batch_load,
        owner_slot,
        atom_coords,
        jnp.transpose(point_coords, (1, 0, 2)),
        charge,
        shell_index,
        jnp.asarray(ghigh),
        jnp.asarray(glow),
    )
    return (potential, moments)


def solution(mesh):
    return jax.shard_map(
        body,
        mesh=mesh,
        in_specs=(
            P(("gx", "gy"), None, None),
            P(("gx", "gy"), None),
            P(("gx", "gy"), None, None),
            P(("gx", "gy"), None),
            P(("gx", "gy")),
            P(("gx", "gy")),
            P(),
            P(),
        ),
        out_specs=(P(("gx", "gy"), None), P(("gx", "gy"), None)),
        check_vma=False,
    )
```

```python
import math

import jax
import jax.numpy as jnp
import numpy as np
from jax import lax
from jax.experimental import pallas as pl
from jax.experimental.pallas import tpu as pltpu
from jax.sharding import PartitionSpec as P

MESH = pl.DeviceIdType.MESH
F32 = jnp.float32
BF16 = jnp.bfloat16
SHELLS = 64
LMAX = 6
LM = 49
KP = 56
SOFTEN = 0.01
ROWS = 11
PITCH = 16
SLOTP = 136
WAVE = 32


def green_pair():
    rank = np.arange(SHELLS, dtype=np.float64)
    radius = 0.5 * np.exp(2.3 * rank / SHELLS)
    nearer = np.minimum(radius[:, None], radius[None, :])
    farther = np.maximum(radius[:, None], radius[None, :])
    full = np.stack(
        [
            4.0 * math.pi / (2 * d + 1) * nearer**d / farther ** (d + 1)
            for d in range(LMAX + 1)
        ]
    )
    full = np.concatenate([full, full], axis=2).astype(np.float32)
    high = full.astype(jnp.bfloat16)
    low = (full - high.astype(np.float32)).astype(jnp.bfloat16)
    return high, low


def split(x):
    high = x.astype(BF16).astype(F32)
    return high, x - high


def dot(a, b, dims=((1,), (0,))):
    return lax.dot_general(a, b, (dims, ((), ())), preferred_element_type=F32)


def harmonics(ux, uy, uz):
    cosine = [None]
    sine = [None]
    for m in range(1, LMAX + 1):
        if m == 1:
            cosine.append(ux)
            sine.append(uy)
        else:
            pc, ps = cosine[-1], sine[-1]
            cosine.append(pc * ux - ps * uy)
            sine.append(pc * uy + ps * ux)

    def norm(d, m):
        value = math.sqrt(
            (2 * d + 1) / (4 * math.pi) * math.factorial(d - m) / math.factorial(d + m)
        )
        return value * (math.sqrt(2.0) if m else 1.0)

    out = {}
    for m in range(LMAX + 1):
        start = norm(m, m) * float(math.prod(range(1, 2 * m, 2)))
        older, old = None, None
        for d in range(m, LMAX + 1):
            if d == m:
                now = start
            elif d == m + 1:
                now = uz * ((2 * m + 1) * start * norm(d, m) / norm(m, m))
            else:
                ca = (2 * d - 1) / (d - m) * norm(d, m) / norm(d - 1, m)
                cb = (d + m - 1) / (d - m) * norm(d, m) / norm(d - 2, m)
                now = (ca * uz) * old - cb * older
            if m == 0:
                out[d * d + d] = now if d else jnp.full(ux.shape, start, F32)
            else:
                out[d * d + d + m] = cosine[m] * now
                out[d * d + d - m] = sine[m] * now
            older, old = old, now
    return out


def visiting_order():
    every = [
        (dy, dz, dx, dc)
        for dy in range(4)
        for dz in range(4)
        for dx in range(4)
        for dc in range(2)
    ]

    def far(t):
        return sum(min(v, 4 - v) for v in t[:3])

    return every[:1] + sorted(every[1:], key=far, reverse=True)


ORDER = visiting_order()


def fused_kernel(
    labels,
    count,
    load,
    owner,
    atoms,
    coords,
    charge,
    shell,
    ghigh,
    glow,
    steps,
    moments,
    mine,
    back,
    place,
    src,
    pay,
    arrived,
    ys,
    ws,
    hots,
    parts,
    acc,
    tables,
    reply,
    send_sem,
    recv_sem,
    reply_send,
    reply_recv,
):
    batches, slots = labels.shape
    spaces = batches * slots
    devices = pay.shape[0]
    owned = moments.shape[0]
    gy = lax.axis_index("gy")
    at = (lax.axis_index("gx"), gy // 8, lax.rem(gy, 8) // 2, lax.rem(gy, 2))
    spans = (4, 4, 4, 2)
    moved_to = [
        [lax.rem(at[axis] + step, spans[axis]) for step in range(spans[axis])]
        for axis in range(4)
    ]

    def peer(i, sign):
        y, z, x, c = [
            moved_to[axis][sign * step % spans[axis]]
            for axis, step in enumerate(ORDER[i])
        ]
        return (y, z * 8 + x * 2 + c)

    barrier = pltpu.get_barrier_semaphore()
    for i in range(1, devices):
        pl.semaphore_signal(
            barrier, inc=1, device_id=peer(i, -1), device_id_type=MESH
        )

    for b in range(batches):

        @pl.loop(0, slots, unroll=4)
        def _(s):
            label = labels[b, s]
            target = owner[label]
            row = b * slots + s
            for c in range(3):
                place[c, pl.ds(row, 1), :] = jnp.full((1, 128), atoms[c, label], F32)
            place[3, pl.ds(row, 1), :] = jnp.full(
                (1, 128), (target // owned).astype(F32), F32
            )
            src[10, pl.ds(row, 1), :] = jnp.full(
                (1, 128), lax.rem(target, owned).astype(F32), F32
            )

    slot_rank = lax.broadcasted_iota(jnp.int32, (slots, 128), 0)
    lane = lax.broadcasted_iota(jnp.int32, (slots, 128), 1)
    lives = []
    for b in range(batches):
        live = jnp.clip(load[0] - b, 0, 1).astype(F32)
        slot_live = jnp.clip(count[b] - slot_rank, 0, 1).astype(F32)
        here = slice(b * slots, (b + 1) * slots)
        lives.append(jnp.where(lane == b, slot_live * live, 0.0))
        for h in range(2):
            points = slice(h * 128, (h + 1) * 128)
            squared = 0.0
            for c in range(3):
                offset = coords[c, b : b + 1, points] - place[c, here, :]
                src[2 * c + h, here, :] = offset
                squared = squared + offset * offset
            closeness = slot_live / (1.0 + squared)
            total = jnp.sum(closeness, axis=0, keepdims=True)
            scaled = charge[b : b + 1, points] * live / total
            src[6 + h, here, :] = shell[b, :, points].astype(F32)
            src[8 + h, here, :] = slot_live * scaled

    row_of = 0
    for axis in range(4):
        there = lax.rem(steps[axis : axis + 1, :] + at[axis], spans[axis])
        row_of = row_of * spans[axis] + there
    goes = (place[3] == row_of.astype(F32)).astype(F32)
    goes = goes.T.astype(BF16)
    flat_pay = pay.reshape(devices * PITCH, 128)
    for r in range(ROWS):
        high, rest = split(src[r])
        moved = dot(goes, high.astype(BF16))
        if r not in (6, 7, 10):
            middle, low = split(rest)
            moved = (
                moved + dot(goes, middle.astype(BF16)) + dot(goes, low.astype(BF16))
            )
        flat_pay[pl.ds(r, devices, stride=PITCH), :] = moved
    lives = dot(goes, jnp.concatenate(lives, axis=0).astype(BF16))
    mine[...] = lives.T[:8]

    pl.semaphore_wait(barrier, devices - 1)

    def piece(ref, i, size=1):
        return ref.at[pl.ds(i, size), pl.ds(0, ROWS)]

    for i in range(1, devices):
        pltpu.make_async_remote_copy(
            src_ref=piece(pay, i),
            dst_ref=piece(arrived, i),
            send_sem=send_sem,
            recv_sem=recv_sem.at[i // WAVE],
            device_id=peer(i, 1),
            device_id_type=MESH,
        ).start()

    arrived[0] = pay[0]
    flat = arrived.reshape(devices * PITCH, 128)
    shell_rank = lax.broadcasted_iota(jnp.int32, (SHELLS, 128), 0).astype(F32)

    def shapes(g):
        for h in range(2):

            def row(r):
                return flat[pl.ds(g * 8 * PITCH + 2 * r + h, 8, stride=PITCH), :]

            dx, dy, dz = row(0), row(1), row(2)
            squared = dx * dx + dy * dy + dz * dz
            scale = lax.rsqrt(squared + SOFTEN)
            ws[h, pl.ds(pl.multiple_of(g * 8, 8), 8), :] = row(4) / (1.0 + squared)
            values = harmonics(dx * scale, dy * scale, dz * scale)
            for k in range(KP):
                value = values[k] if k < LM else jnp.zeros_like(dx)
                ys[h, pl.ds(g * 8 * KP + k, 8, stride=KP), :] = value

    def forward(i):
        stack, hot = [], []
        for h in range(2):
            y = ys[h, pl.ds(pl.multiple_of(i * KP, 8), KP), :]
            weighted = y * ws[h, pl.ds(i, 1), :]
            high, low = split(weighted)
            stack.append(jnp.concatenate([high, low], axis=0).astype(BF16))
            shells = flat[pl.ds(i * PITCH + 6 + h, 1), :]
            hot.append((shells == shell_rank).astype(F32).astype(BF16))
        hot = jnp.concatenate(hot, axis=1)
        hots[i] = hot
        both = dot(jnp.concatenate(stack, axis=1), hot, ((1,), (1,)))
        parts[pl.ds(i, KP, stride=SLOTP), :SHELLS] = both[:KP] + both[KP:]

    def landed(g, size):
        pltpu.make_async_remote_copy(
            src_ref=piece(pay, 1, size),
            dst_ref=piece(arrived, 1, size),
            send_sem=send_sem,
            recv_sem=recv_sem.at[g],
            device_id=(0, 0),
            device_id_type=MESH,
        ).wait_recv()

    @pl.loop(0, devices // WAVE)
    def _(g):
        @pl.when(g == 0)
        def _():
            landed(g, WAVE - 1)

        @pl.when(g > 0)
        def _():
            landed(g, WAVE)

        @pl.loop(0, WAVE // 8)
        def _(q):
            shapes(g * (WAVE // 8) + q)

        for e in range(WAVE):
            forward(g * WAVE + e)

    marks = flat[pl.ds(10, devices, stride=PITCH), :]
    picks = (
        marks == lax.broadcasted_iota(jnp.int32, (devices, 128), 1).astype(F32)
    ).astype(F32)
    gather = picks[:, :owned].astype(BF16)
    combine = picks.T[:owned].astype(BF16)
    combine = jnp.concatenate([combine, combine], axis=1)
    for k in range(LM):
        high, low = split(parts[pl.ds(k * SLOTP, devices), :SHELLS])
        both = jnp.concatenate([high, low], axis=0).astype(BF16)
        acc[k * owned : (k + 1) * owned, :SHELLS] = dot(combine, both)

    for d in range(LMAX + 1):
        begin, end = d * d, (d + 1) * (d + 1)
        high, low = split(acc[begin * owned : end * owned, :SHELLS])
        high, low = high.astype(BF16), low.astype(BF16)
        table = dot(high, ghigh[d]) + dot(low, ghigh[d]) + dot(high, glow[d])
        thigh, tlow = split(table)
        lane_rank = lax.broadcasted_iota(jnp.int32, table.shape, 1)
        table = jnp.where(lane_rank < SHELLS, thigh, tlow).astype(BF16)
        for k in range(begin, end):
            tables[k * SLOTP : k * SLOTP + devices, :] = dot(
                gather, table[(k - begin) * owned : (k - begin + 1) * owned]
            )
    for k in range(LM, KP):
        tables[k * SLOTP : k * SLOTP + devices, :] = jnp.zeros((devices, 128), F32)

    def evaluate(i):
        table = tables[pl.ds(i, KP, stride=SLOTP), :].astype(BF16)
        hot = hots[i]
        picked = dot(table, jnp.concatenate([hot, hot], axis=0))
        for h in range(2):
            y = ys[h, pl.ds(pl.multiple_of(i * KP, 8), KP), :]
            total = jnp.sum(
                picked[:, h * 128 : (h + 1) * 128] * y, axis=0, keepdims=True
            )
            reply[i, h : h + 1, :] = total

    def answer(g):
        for i in range(max(g * WAVE, 1), (g + 1) * WAVE):
            pltpu.make_async_remote_copy(
                src_ref=reply.at[i],
                dst_ref=back.at[i],
                send_sem=reply_send,
                recv_sem=reply_recv,
                device_id=peer(i, -1),
                device_id_type=MESH,
            ).start()

    for g in range(devices // WAVE):
        for e in range(WAVE):
            evaluate(g * WAVE + e)
        if g:
            answer(g - 1)
    back[0] = reply[0]
    answer(devices // WAVE - 1)
    for k in range(0, LM, 2):
        first = acc[k * owned : (k + 1) * owned, :SHELLS]
        if k + 1 < LM:
            second = acc[(k + 1) * owned : (k + 2) * owned, :SHELLS]
            first = jnp.concatenate([first, second], axis=1)
        moments[:, k * SHELLS : min(k + 2, LM) * SHELLS] = first

    everything = pltpu.make_async_remote_copy(
        src_ref=piece(pay, 1, devices - 1),
        dst_ref=piece(arrived, 1, devices - 1),
        send_sem=send_sem,
        recv_sem=recv_sem.at[0],
        device_id=(0, 0),
        device_id_type=MESH,
    )
    everything.wait_send()
    answers = pltpu.make_async_remote_copy(
        src_ref=reply.at[pl.ds(1, devices - 1)],
        dst_ref=back.at[pl.ds(1, devices - 1)],
        send_sem=reply_send,
        recv_sem=reply_recv,
        device_id=(0, 0),
        device_id_type=MESH,
    )
    answers.wait_send()
    answers.wait_recv()


def finish_kernel(mine, back, sums, potential, moments):
    batches = potential.shape[0]
    chosen = mine[...].astype(BF16)
    for h in range(2):
        high, rest = split(back[:, h, :])
        middle, low = split(rest)
        total = (
            dot(chosen, high.astype(BF16))
            + dot(chosen, middle.astype(BF16))
            + dot(chosen, low.astype(BF16))
        )
        potential[:, h * 128 : (h + 1) * 128] = total[:batches]
    moments[...] = sums[...]


VMEM = pl.BlockSpec(memory_space=pltpu.VMEM)
SMEM = pl.BlockSpec(memory_space=pltpu.SMEM)


def body(
    point_coords,
    charge,
    shell_index,
    neighbours,
    neighbour_count,
    batch_load,
    atom_coords,
    owner_slot,
):
    batches = charge.shape[0]
    slots = neighbours.shape[1]
    devices = lax.axis_size("gx") * lax.axis_size("gy")
    owned = owner_slot.shape[0] // devices
    spaces = batches * slots
    sds = jax.ShapeDtypeStruct
    ghigh, glow = green_pair()
    sums, mine, back = pl.pallas_call(
        fused_kernel,
        out_shape=(
            sds((owned, LM * SHELLS), F32),
            sds((8, devices), F32),
            sds((devices, 2, 128), F32),
        ),
        in_specs=[SMEM] * 5 + [VMEM] * 6,
        out_specs=(VMEM, VMEM, VMEM),
        scratch_shapes=[
            pltpu.VMEM((4, spaces, 128), F32),
            pltpu.VMEM((ROWS, spaces, 128), F32),
            pltpu.VMEM((devices, PITCH, 128), F32),
            pltpu.VMEM((devices, PITCH, 128), F32),
            pltpu.VMEM((2, devices * KP, 128), F32),
            pltpu.VMEM((2, devices, 128), F32),
            pltpu.VMEM((devices, SHELLS, 256), BF16),
            pltpu.VMEM((KP * SLOTP, 128), F32),
            pltpu.VMEM((LM * owned, 128), F32),
            pltpu.VMEM((KP * SLOTP, 128), F32),
            pltpu.VMEM((devices, 2, 128), F32),
            pltpu.SemaphoreType.DMA,
            pltpu.SemaphoreType.DMA((devices // WAVE,)),
            pltpu.SemaphoreType.DMA,
            pltpu.SemaphoreType.DMA,
        ],
        compiler_params=pltpu.CompilerParams(collective_id=0, has_side_effects=True),
        name="fused",
    )(
        neighbours,
        neighbour_count,
        batch_load,
        owner_slot,
        atom_coords,
        jnp.transpose(point_coords, (1, 0, 2)),
        charge,
        shell_index,
        jnp.asarray(ghigh),
        jnp.asarray(glow),
        jnp.asarray(np.array(ORDER, dtype=np.int32).T),
    )
    potential, moments = pl.pallas_call(
        finish_kernel,
        out_shape=(sds(charge.shape, F32), sds(sums.shape, F32)),
        in_specs=[VMEM] * 3,
        out_specs=(VMEM, VMEM),
        name="finish",
    )(mine, back, sums)
    return (potential, moments)


def solution(mesh):
    return jax.shard_map(
        body,
        mesh=mesh,
        in_specs=(
            P(("gx", "gy"), None, None),
            P(("gx", "gy"), None),
            P(("gx", "gy"), None, None),
            P(("gx", "gy"), None),
            P(("gx", "gy")),
            P(("gx", "gy")),
            P(),
            P(),
        ),
        out_specs=(P(("gx", "gy"), None), P(("gx", "gy"), None)),
        check_vma=False,
    )
```

```python
import math

import jax
import jax.numpy as jnp
import numpy as np
from jax import lax
from jax.experimental import pallas as pl
from jax.experimental.pallas import tpu as pltpu
from jax.sharding import PartitionSpec as P

MESH = pl.DeviceIdType.MESH
F32 = jnp.float32
BF16 = jnp.bfloat16
SHELLS = 64
LMAX = 6
LM = 49
KP = 56
SOFTEN = 0.01
ROWS = 11
PITCH = 16
SLOTP = 136
WAVE = 32


def green_pair():
    rank = np.arange(SHELLS, dtype=np.float64)
    radius = 0.5 * np.exp(2.3 * rank / SHELLS)
    nearer = np.minimum(radius[:, None], radius[None, :])
    farther = np.maximum(radius[:, None], radius[None, :])
    full = np.stack(
        [
            4.0 * math.pi / (2 * d + 1) * nearer**d / farther ** (d + 1)
            for d in range(LMAX + 1)
        ]
    )
    full = np.concatenate([full, full], axis=2).astype(np.float32)
    high = full.astype(jnp.bfloat16)
    low = (full - high.astype(np.float32)).astype(jnp.bfloat16)
    return high, low


def split(x):
    high = x.astype(BF16).astype(F32)
    return high, x - high


def dot(a, b, dims=((1,), (0,))):
    return lax.dot_general(a, b, (dims, ((), ())), preferred_element_type=F32)


def harmonics(ux, uy, uz):
    cosine = [None]
    sine = [None]
    for m in range(1, LMAX + 1):
        if m == 1:
            cosine.append(ux)
            sine.append(uy)
        else:
            pc, ps = cosine[-1], sine[-1]
            cosine.append(pc * ux - ps * uy)
            sine.append(pc * uy + ps * ux)

    def norm(d, m):
        value = math.sqrt(
            (2 * d + 1) / (4 * math.pi) * math.factorial(d - m) / math.factorial(d + m)
        )
        return value * (math.sqrt(2.0) if m else 1.0)

    out = {}
    for m in range(LMAX + 1):
        start = norm(m, m) * float(math.prod(range(1, 2 * m, 2)))
        older, old = None, None
        for d in range(m, LMAX + 1):
            if d == m:
                now = start
            elif d == m + 1:
                now = uz * ((2 * m + 1) * start * norm(d, m) / norm(m, m))
            else:
                ca = (2 * d - 1) / (d - m) * norm(d, m) / norm(d - 1, m)
                cb = (d + m - 1) / (d - m) * norm(d, m) / norm(d - 2, m)
                now = (ca * uz) * old - cb * older
            if m == 0:
                out[d * d + d] = now if d else jnp.full(ux.shape, start, F32)
            else:
                out[d * d + d + m] = cosine[m] * now
                out[d * d + d - m] = sine[m] * now
            older, old = old, now
    return out


def visiting_order():
    every = [
        (dy, dz, dx, dc)
        for dy in range(4)
        for dz in range(4)
        for dx in range(4)
        for dc in range(2)
    ]

    def far(t):
        return sum(min(v, 4 - v) for v in t[:3])

    return every[:1] + sorted(every[1:], key=far, reverse=True)


ORDER = visiting_order()


def fused_kernel(
    *refs,
):
    load, given, refs = refs[0], refs[1:11], refs[11:]
    sums, mine, back = refs[:3]
    held, refs = refs[3:13], refs[13:]
    (
        place,
        src,
        pay,
        arrived,
        ys,
        ws,
        hots,
        parts,
        acc,
        tables,
        reply,
        load_sem,
        send_sem,
        recv_sem,
        reply_send,
        reply_recv,
    ) = refs
    labels, count, owner, atoms, coords, charge, shell, ghigh, glow, steps = held
    loads = [
        pltpu.make_async_copy(given[n], held[n], load_sem.at[n])
        for n in range(len(held))
    ]
    for one in loads:
        one.start()
    batches, slots = labels.shape
    spaces = batches * slots
    devices = pay.shape[0]
    owned = sums.shape[0]
    gy = lax.axis_index("gy")
    at = (lax.axis_index("gx"), gy // 8, lax.rem(gy, 8) // 2, lax.rem(gy, 2))
    spans = (4, 4, 4, 2)
    moved_to = [
        [lax.rem(at[axis] + step, spans[axis]) for step in range(spans[axis])]
        for axis in range(4)
    ]

    def peer(i, sign):
        y, z, x, c = [
            moved_to[axis][sign * step % spans[axis]]
            for axis, step in enumerate(ORDER[i])
        ]
        return (y, z * 8 + x * 2 + c)

    barrier = pltpu.get_barrier_semaphore()
    for i in range(1, devices):
        pl.semaphore_signal(
            barrier, inc=1, device_id=peer(i, -1), device_id_type=MESH
        )

    for one in loads:
        one.wait()
    for b in range(batches):

        @pl.loop(0, slots, unroll=4)
        def _(s):
            label = labels[b, s]
            target = owner[label]
            row = b * slots + s
            for c in range(3):
                place[c, pl.ds(row, 1), :] = jnp.full((1, 128), atoms[c, label], F32)
            place[3, pl.ds(row, 1), :] = jnp.full(
                (1, 128), (target // owned).astype(F32), F32
            )
            src[10, pl.ds(row, 1), :] = jnp.full(
                (1, 128), lax.rem(target, owned).astype(F32), F32
            )

    slot_rank = lax.broadcasted_iota(jnp.int32, (slots, 128), 0)
    lane = lax.broadcasted_iota(jnp.int32, (slots, 128), 1)
    lives = []
    for b in range(batches):
        live = jnp.clip(load[0] - b, 0, 1).astype(F32)
        slot_live = jnp.clip(count[b] - slot_rank, 0, 1).astype(F32)
        here = slice(b * slots, (b + 1) * slots)
        lives.append(jnp.where(lane == b, slot_live * live, 0.0))
        for h in range(2):
            points = slice(h * 128, (h + 1) * 128)
            squared = 0.0
            for c in range(3):
                offset = coords[c, b : b + 1, points] - place[c, here, :]
                src[2 * c + h, here, :] = offset
                squared = squared + offset * offset
            closeness = slot_live / (1.0 + squared)
            total = jnp.sum(closeness, axis=0, keepdims=True)
            scaled = charge[b : b + 1, points] * live / total
            src[6 + h, here, :] = shell[b, :, points].astype(F32)
            src[8 + h, here, :] = slot_live * scaled

    row_of = 0
    for axis in range(4):
        there = lax.rem(steps[axis : axis + 1, :] + at[axis], spans[axis])
        row_of = row_of * spans[axis] + there
    goes = (place[3] == row_of.astype(F32)).astype(F32)
    goes = goes.T.astype(BF16)
    flat_pay = pay.reshape(devices * PITCH, 128)
    for r in range(ROWS):
        high, rest = split(src[r])
        moved = dot(goes, high.astype(BF16))
        if r not in (6, 7, 10):
            middle, low = split(rest)
            moved = (
                moved + dot(goes, middle.astype(BF16)) + dot(goes, low.astype(BF16))
            )
        flat_pay[pl.ds(r, devices, stride=PITCH), :] = moved
    lives = dot(goes, jnp.concatenate(lives, axis=0).astype(BF16))
    mine[...] = lives.T[:8]

    pl.semaphore_wait(barrier, devices - 1)

    def piece(ref, i, size=1):
        return ref.at[pl.ds(i, size), pl.ds(0, ROWS)]

    for i in range(1, devices):
        pltpu.make_async_remote_copy(
            src_ref=piece(pay, i),
            dst_ref=piece(arrived, i),
            send_sem=send_sem,
            recv_sem=recv_sem.at[i // WAVE],
            device_id=peer(i, 1),
            device_id_type=MESH,
        ).start()

    arrived[0] = pay[0]
    flat = arrived.reshape(devices * PITCH, 128)
    shell_rank = lax.broadcasted_iota(jnp.int32, (SHELLS, 128), 0).astype(F32)

    def shapes(g):
        for h in range(2):

            def row(r):
                return flat[pl.ds(g * 8 * PITCH + 2 * r + h, 8, stride=PITCH), :]

            dx, dy, dz = row(0), row(1), row(2)
            squared = dx * dx + dy * dy + dz * dz
            scale = lax.rsqrt(squared + SOFTEN)
            ws[h, pl.ds(pl.multiple_of(g * 8, 8), 8), :] = row(4) / (1.0 + squared)
            values = harmonics(dx * scale, dy * scale, dz * scale)
            for k in range(KP):
                value = values[k] if k < LM else jnp.zeros_like(dx)
                ys[h, pl.ds(g * 8 * KP + k, 8, stride=KP), :] = value

    def forward(i):
        stack, hot = [], []
        for h in range(2):
            y = ys[h, pl.ds(pl.multiple_of(i * KP, 8), KP), :]
            weighted = y * ws[h, pl.ds(i, 1), :]
            high, low = split(weighted)
            stack.append(jnp.concatenate([high, low], axis=0).astype(BF16))
            shells = flat[pl.ds(i * PITCH + 6 + h, 1), :]
            hot.append((shells == shell_rank).astype(F32).astype(BF16))
        hot = jnp.concatenate(hot, axis=1)
        hots[i] = hot
        both = dot(jnp.concatenate(stack, axis=1), hot, ((1,), (1,)))
        parts[pl.ds(i, KP, stride=SLOTP), :SHELLS] = both[:KP] + both[KP:]

    def landed(g, size):
        pltpu.make_async_remote_copy(
            src_ref=piece(pay, 1, size),
            dst_ref=piece(arrived, 1, size),
            send_sem=send_sem,
            recv_sem=recv_sem.at[g],
            device_id=(0, 0),
            device_id_type=MESH,
        ).wait_recv()

    @pl.loop(0, devices // WAVE)
    def _(g):
        @pl.when(g == 0)
        def _():
            landed(g, WAVE - 1)

        @pl.when(g > 0)
        def _():
            landed(g, WAVE)

        @pl.loop(0, WAVE // 8)
        def _(q):
            shapes(g * (WAVE // 8) + q)

        for e in range(WAVE):
            forward(g * WAVE + e)

    marks = flat[pl.ds(10, devices, stride=PITCH), :]
    picks = (
        marks == lax.broadcasted_iota(jnp.int32, (devices, 128), 1).astype(F32)
    ).astype(F32)
    gather = picks[:, :owned].astype(BF16)
    combine = picks.T[:owned].astype(BF16)
    combine = jnp.concatenate([combine, combine], axis=1)
    for k in range(LM):
        high, low = split(parts[pl.ds(k * SLOTP, devices), :SHELLS])
        both = jnp.concatenate([high, low], axis=0).astype(BF16)
        acc[k * owned : (k + 1) * owned, :SHELLS] = dot(combine, both)

    for d in range(LMAX + 1):
        begin, end = d * d, (d + 1) * (d + 1)
        high, low = split(acc[begin * owned : end * owned, :SHELLS])
        high, low = high.astype(BF16), low.astype(BF16)
        table = dot(high, ghigh[d]) + dot(low, ghigh[d]) + dot(high, glow[d])
        thigh, tlow = split(table)
        lane_rank = lax.broadcasted_iota(jnp.int32, table.shape, 1)
        table = jnp.where(lane_rank < SHELLS, thigh, tlow).astype(BF16)
        for k in range(begin, end, 2):
            rows = [
                table[(n - begin) * owned : (n - begin + 1) * owned]
                for n in range(k, min(k + 2, end))
            ]
            picked = dot(gather, jnp.concatenate(rows, axis=1))
            for n in range(len(rows)):
                at_k = (k + n) * SLOTP
                tables[at_k : at_k + devices, :] = picked[:, n * 128 : (n + 1) * 128]
    for k in range(LM, KP):
        tables[k * SLOTP : k * SLOTP + devices, :] = jnp.zeros((devices, 128), F32)

    def evaluate(i):
        table = tables[pl.ds(i, KP, stride=SLOTP), :].astype(BF16)
        hot = hots[i]
        picked = dot(table, jnp.concatenate([hot, hot], axis=0))
        for h in range(2):
            y = ys[h, pl.ds(pl.multiple_of(i * KP, 8), KP), :]
            total = jnp.sum(
                picked[:, h * 128 : (h + 1) * 128] * y, axis=0, keepdims=True
            )
            reply[i, h : h + 1, :] = total

    def answer(begin, end):
        for i in range(max(begin, 1), end):
            pltpu.make_async_remote_copy(
                src_ref=reply.at[i],
                dst_ref=back.at[i],
                send_sem=reply_send,
                recv_sem=reply_recv,
                device_id=peer(i, -1),
                device_id_type=MESH,
            ).start()

    cuts = (0, 16, 32, 64, 96, devices)
    for n in range(len(cuts) - 1):
        for i in range(cuts[n], cuts[n + 1]):
            evaluate(i)
        if n:
            answer(cuts[n - 1], cuts[n])
    back[0] = reply[0]
    answer(cuts[-2], cuts[-1])
    for k in range(0, LM, 2):
        first = acc[k * owned : (k + 1) * owned, :SHELLS]
        if k + 1 < LM:
            second = acc[(k + 1) * owned : (k + 2) * owned, :SHELLS]
            first = jnp.concatenate([first, second], axis=1)
        sums[:, k * SHELLS : min(k + 2, LM) * SHELLS] = first

    everything = pltpu.make_async_remote_copy(
        src_ref=piece(pay, 1, devices - 1),
        dst_ref=piece(arrived, 1, devices - 1),
        send_sem=send_sem,
        recv_sem=recv_sem.at[0],
        device_id=(0, 0),
        device_id_type=MESH,
    )
    everything.wait_send()
    answers = pltpu.make_async_remote_copy(
        src_ref=reply.at[pl.ds(1, devices - 1)],
        dst_ref=back.at[pl.ds(1, devices - 1)],
        send_sem=reply_send,
        recv_sem=reply_recv,
        device_id=(0, 0),
        device_id_type=MESH,
    )
    answers.wait_send()
    answers.wait_recv()


def finish_kernel(mine, back, sums, potential, moments):
    batches = potential.shape[0]
    chosen = mine[...].astype(BF16)
    for h in range(2):
        high, rest = split(back[:, h, :])
        middle, low = split(rest)
        total = (
            dot(chosen, high.astype(BF16))
            + dot(chosen, middle.astype(BF16))
            + dot(chosen, low.astype(BF16))
        )
        potential[:, h * 128 : (h + 1) * 128] = total[:batches]
    moments[...] = sums[...]


VMEM = pl.BlockSpec(memory_space=pltpu.VMEM)
HBM = pl.BlockSpec(memory_space=pltpu.HBM)
SMEM = pl.BlockSpec(memory_space=pltpu.SMEM)


def body(
    point_coords,
    charge,
    shell_index,
    neighbours,
    neighbour_count,
    batch_load,
    atom_coords,
    owner_slot,
):
    batches, points = charge.shape
    slots = neighbours.shape[1]
    devices = lax.axis_size("gx") * lax.axis_size("gy")
    owned = owner_slot.shape[0] // devices
    spaces = batches * slots
    sds = jax.ShapeDtypeStruct
    ghigh, glow = green_pair()
    sums, mine, back = pl.pallas_call(
        fused_kernel,
        out_shape=(
            sds((owned, LM * SHELLS), F32),
            sds((8, devices), F32),
            sds((devices, 2, 128), F32),
        ),
        in_specs=[SMEM] + [HBM] * 10,
        out_specs=(VMEM, VMEM, VMEM),
        scratch_shapes=[
            pltpu.SMEM((batches, slots), jnp.int32),
            pltpu.SMEM((batches,), jnp.int32),
            pltpu.SMEM(owner_slot.shape, jnp.int32),
            pltpu.SMEM(atom_coords.shape, F32),
            pltpu.VMEM((3, batches, points), F32),
            pltpu.VMEM((batches, points), F32),
            pltpu.VMEM((batches, slots, points), jnp.int32),
            pltpu.VMEM(ghigh.shape, BF16),
            pltpu.VMEM(glow.shape, BF16),
            pltpu.VMEM((4, devices), jnp.int32),
            pltpu.VMEM((4, spaces, 128), F32),
            pltpu.VMEM((ROWS, spaces, 128), F32),
            pltpu.VMEM((devices, PITCH, 128), F32),
            pltpu.VMEM((devices, PITCH, 128), F32),
            pltpu.VMEM((2, devices * KP, 128), F32),
            pltpu.VMEM((2, devices, 128), F32),
            pltpu.VMEM((devices, SHELLS, 256), BF16),
            pltpu.VMEM((KP * SLOTP, 128), F32),
            pltpu.VMEM((LM * owned, 128), F32),
            pltpu.VMEM((KP * SLOTP, 128), F32),
            pltpu.VMEM((devices, 2, 128), F32),
            pltpu.SemaphoreType.DMA((10,)),
            pltpu.SemaphoreType.DMA,
            pltpu.SemaphoreType.DMA((devices // WAVE,)),
            pltpu.SemaphoreType.DMA,
            pltpu.SemaphoreType.DMA,
        ],
        compiler_params=pltpu.CompilerParams(
            collective_id=0, has_side_effects=True, vmem_limit_bytes=34 << 20
        ),
        name="fused",
    )(
        batch_load,
        *[
            pltpu.with_memory_space_constraint(one, pltpu.HBM)
            for one in (
                neighbours,
                neighbour_count,
                owner_slot,
                atom_coords,
                jnp.transpose(point_coords, (1, 0, 2)),
                charge,
                shell_index,
                jnp.asarray(ghigh),
                jnp.asarray(glow),
                jnp.asarray(np.array(ORDER, dtype=np.int32).T),
            )
        ]
    )
    potential, moments = pl.pallas_call(
        finish_kernel,
        out_shape=(sds(charge.shape, F32), sds(sums.shape, F32)),
        in_specs=[VMEM] * 3,
        out_specs=(VMEM, VMEM),
        compiler_params=pltpu.CompilerParams(vmem_limit_bytes=4 << 20),
        name="finish",
    )(mine, back, sums)
    return (potential, moments)


def solution(mesh):
    return jax.shard_map(
        body,
        mesh=mesh,
        in_specs=(
            P(("gx", "gy"), None, None),
            P(("gx", "gy"), None),
            P(("gx", "gy"), None, None),
            P(("gx", "gy"), None),
            P(("gx", "gy")),
            P(("gx", "gy")),
            P(),
            P(),
        ),
        out_specs=(P(("gx", "gy"), None), P(("gx", "gy"), None)),
        check_vma=False,
    )
```

```python
import math

import jax
import jax.numpy as jnp
import numpy as np
from jax import lax
from jax.experimental import pallas as pl
from jax.experimental.pallas import tpu as pltpu
from jax.sharding import PartitionSpec as P

MESH = pl.DeviceIdType.MESH
F32 = jnp.float32
BF16 = jnp.bfloat16
SHELLS = 64
LMAX = 6
LM = 49
KP = 56
HALF = 24
SOFTEN = 0.01
ROWS = 11
PITCH = 16
SLOTP = 136
WAVE = 32


def green_blocks():
    rank = np.arange(SHELLS, dtype=np.float64)
    radius = 0.5 * np.exp(2.3 * rank / SHELLS)
    nearer = np.minimum(radius[:, None], radius[None, :])
    farther = np.maximum(radius[:, None], radius[None, :])
    full = np.stack(
        [
            4.0 * math.pi / (2 * d + 1) * nearer**d / farther ** (d + 1)
            for d in range(LMAX + 1)
        ]
    )
    full = np.concatenate([full, full], axis=2).astype(np.float32)
    high = full.astype(jnp.bfloat16)
    low = (full - high.astype(np.float32)).astype(jnp.bfloat16)
    upper = np.concatenate([high, low], axis=2)
    lower = np.concatenate([high, np.zeros_like(low)], axis=2)
    return np.concatenate([upper, lower], axis=1)


def split(x):
    high = x.astype(BF16).astype(F32)
    return high, x - high


def dot(a, b, dims=((1,), (0,))):
    return lax.dot_general(a, b, (dims, ((), ())), preferred_element_type=F32)


def harmonics(ux, uy, uz):
    cosine = [None]
    sine = [None]
    for m in range(1, LMAX + 1):
        if m == 1:
            cosine.append(ux)
            sine.append(uy)
        else:
            pc, ps = cosine[-1], sine[-1]
            cosine.append(pc * ux - ps * uy)
            sine.append(pc * uy + ps * ux)

    def norm(d, m):
        value = math.sqrt(
            (2 * d + 1) / (4 * math.pi) * math.factorial(d - m) / math.factorial(d + m)
        )
        return value * (math.sqrt(2.0) if m else 1.0)

    out = {}
    for m in range(LMAX + 1):
        start = norm(m, m) * float(math.prod(range(1, 2 * m, 2)))
        older, old = None, None
        for d in range(m, LMAX + 1):
            if d == m:
                now = start
            elif d == m + 1:
                now = uz * ((2 * m + 1) * start * norm(d, m) / norm(m, m))
            else:
                ca = (2 * d - 1) / (d - m) * norm(d, m) / norm(d - 1, m)
                cb = (d + m - 1) / (d - m) * norm(d, m) / norm(d - 2, m)
                now = (ca * uz) * old - cb * older
            if m == 0:
                out[d * d + d] = now if d else jnp.full(ux.shape, start, F32)
            else:
                out[d * d + d + m] = cosine[m] * now
                out[d * d + d - m] = sine[m] * now
            older, old = old, now
    return out


def visiting_order():
    every = [
        (dy, dz, dx, dc)
        for dy in range(4)
        for dz in range(4)
        for dx in range(4)
        for dc in range(2)
    ]

    def far(t):
        return sum(min(v, 4 - v) for v in t[:3])

    return every[:1] + sorted(every[1:], key=far, reverse=True)


ORDER = visiting_order()


def fused_kernel(
    *refs,
):
    load, given, refs = refs[0], refs[1:10], refs[10:]
    sums, mine, back = refs[:3]
    held, refs = refs[3:12], refs[12:]
    (
        place,
        src,
        pay,
        arrived,
        ys,
        ws,
        hots,
        parts,
        acc,
        small,
        tables,
        reply,
        load_sem,
        send_sem,
        recv_sem,
        reply_send,
        reply_recv,
    ) = refs
    labels, count, owner, atoms, coords, charge, shell, green, steps = held
    loads = [
        pltpu.make_async_copy(given[n], held[n], load_sem.at[n])
        for n in range(len(held))
    ]
    for one in loads:
        one.start()
    batches, slots = labels.shape
    spaces = batches * slots
    devices = pay.shape[0]
    owned = sums.shape[0]
    gy = lax.axis_index("gy")
    at = (lax.axis_index("gx"), gy // 8, lax.rem(gy, 8) // 2, lax.rem(gy, 2))
    spans = (4, 4, 4, 2)
    moved_to = [
        [lax.rem(at[axis] + step, spans[axis]) for step in range(spans[axis])]
        for axis in range(4)
    ]

    def peer(i, sign):
        y, z, x, c = [
            moved_to[axis][sign * step % spans[axis]]
            for axis, step in enumerate(ORDER[i])
        ]
        return (y, z * 8 + x * 2 + c)

    barrier = pltpu.get_barrier_semaphore()
    for i in range(1, devices):
        pl.semaphore_signal(
            barrier, inc=1, device_id=peer(i, -1), device_id_type=MESH
        )

    top = jnp.where(
        lax.broadcasted_iota(jnp.int32, (8, 128), 0) == 0,
        math.sqrt(1 / (4 * math.pi)),
        0.0,
    ).astype(F32)

    @pl.loop(0, devices)
    def _(i):
        for h in range(2):
            ys[h, pl.ds(pl.multiple_of(i * KP, 8), 8), :] = top
            ys[h, pl.ds(pl.multiple_of(i * KP + KP - 8, 8), 8), :] = jnp.zeros_like(top)

    for k in range(LM, KP):
        tables[k * SLOTP : k * SLOTP + devices, :] = jnp.zeros((devices, 128), F32)
    parts[(HALF * SLOTP) :, :] = jnp.zeros((SLOTP, 128), F32)

    for one in loads:
        one.wait()
    for b in range(batches):

        @pl.loop(0, slots, unroll=4)
        def _(s):
            label = labels[b, s]
            target = owner[label]
            row = b * slots + s
            for c in range(3):
                place[c, pl.ds(row, 1), :] = jnp.full((1, 128), atoms[c, label], F32)
            place[3, pl.ds(row, 1), :] = jnp.full(
                (1, 128), (target // owned).astype(F32), F32
            )
            src[10, pl.ds(row, 1), :] = jnp.full(
                (1, 128), lax.rem(target, owned).astype(F32), F32
            )

    slot_rank = lax.broadcasted_iota(jnp.int32, (slots, 128), 0)
    lane = lax.broadcasted_iota(jnp.int32, (slots, 128), 1)
    lives = []
    for b in range(batches):
        live = jnp.clip(load[0] - b, 0, 1).astype(F32)
        slot_live = jnp.clip(count[b] - slot_rank, 0, 1).astype(F32)
        here = slice(b * slots, (b + 1) * slots)
        lives.append(jnp.where(lane == b, slot_live * live, 0.0))
        for h in range(2):
            points = slice(h * 128, (h + 1) * 128)
            squared = 0.0
            for c in range(3):
                offset = coords[c, b : b + 1, points] - place[c, here, :]
                src[2 * c + h, here, :] = offset
                squared = squared + offset * offset
            closeness = slot_live / (1.0 + squared)
            total = jnp.sum(closeness, axis=0, keepdims=True)
            scaled = charge[b : b + 1, points] * live / total
            src[6 + h, here, :] = shell[b, :, points].astype(F32)
            src[8 + h, here, :] = slot_live * scaled

    row_of = 0
    for axis in range(4):
        there = lax.rem(steps[axis : axis + 1, :] + at[axis], spans[axis])
        row_of = row_of * spans[axis] + there
    goes = (place[3] == row_of.astype(F32)).astype(F32)
    goes = goes.T.astype(BF16)
    flat_pay = pay.reshape(devices * PITCH, 128)
    for r in range(ROWS):
        high, rest = split(src[r])
        moved = dot(goes, high.astype(BF16))
        if r not in (6, 7, 10):
            middle, low = split(rest)
            moved = (
                moved + dot(goes, middle.astype(BF16)) + dot(goes, low.astype(BF16))
            )
        flat_pay[pl.ds(r, devices, stride=PITCH), :] = moved
    lives = dot(goes, jnp.concatenate(lives, axis=0).astype(BF16))
    mine[...] = lives.T[:8]

    pl.semaphore_wait(barrier, devices - 1)

    def piece(ref, i, size=1):
        return ref.at[pl.ds(i, size), pl.ds(0, ROWS)]

    for i in range(1, devices):
        pltpu.make_async_remote_copy(
            src_ref=piece(pay, i),
            dst_ref=piece(arrived, i),
            send_sem=send_sem,
            recv_sem=recv_sem.at[i // WAVE],
            device_id=peer(i, 1),
            device_id_type=MESH,
        ).start()

    arrived[0] = pay[0]
    flat = arrived.reshape(devices * PITCH, 128)
    shell_rank = lax.broadcasted_iota(jnp.int32, (SHELLS, 128), 0).astype(F32)

    def shapes(g):
        for h in range(2):

            def row(r):
                return flat[pl.ds(g * 8 * PITCH + 2 * r + h, 8, stride=PITCH), :]

            dx, dy, dz = row(0), row(1), row(2)
            squared = dx * dx + dy * dy + dz * dz
            scale = lax.rsqrt(squared + SOFTEN)
            ws[h, pl.ds(pl.multiple_of(g * 8, 8), 8), :] = row(4) / (1.0 + squared)
            values = harmonics(dx * scale, dy * scale, dz * scale)
            for k in range(1, LM):
                ys[h, pl.ds(g * 8 * KP + k, 8, stride=KP), :] = values[k]

    def forward(i):
        stack, hot = [], []
        for h in range(2):
            y = ys[h, pl.ds(pl.multiple_of(i * KP, 8), KP), :]
            weighted = y * ws[h, pl.ds(i, 1), :]
            high, low = split(weighted)
            stack.append(jnp.concatenate([high, low], axis=0).astype(BF16))
            shells = flat[pl.ds(i * PITCH + 6 + h, 1), :]
            hot.append((shells == shell_rank).astype(F32).astype(BF16))
        hot = jnp.concatenate(hot, axis=1)
        hots[i] = hot
        both = dot(jnp.concatenate(stack, axis=1), hot, ((1,), (1,)))
        part = both[:KP] + both[KP:]
        parts[pl.ds(i, HALF, stride=SLOTP), :] = jnp.concatenate(
            [part[:HALF], part[HALF : 2 * HALF]], axis=1
        )
        parts[pl.ds(HALF * SLOTP + i, 1), :SHELLS] = part[2 * HALF : LM]

    def landed(g, size):
        pltpu.make_async_remote_copy(
            src_ref=piece(pay, 1, size),
            dst_ref=piece(arrived, 1, size),
            send_sem=send_sem,
            recv_sem=recv_sem.at[g],
            device_id=(0, 0),
            device_id_type=MESH,
        ).wait_recv()

    @pl.loop(0, devices // WAVE)
    def _(g):
        @pl.when(g == 0)
        def _():
            landed(g, WAVE - 1)

        @pl.when(g > 0)
        def _():
            landed(g, WAVE)

        for q in range(WAVE // 8):
            shapes(g * (WAVE // 8) + q)

        for e in range(WAVE):
            forward(g * WAVE + e)

    marks = flat[pl.ds(10, devices, stride=PITCH), :]
    picks = (
        marks == lax.broadcasted_iota(jnp.int32, (devices, 128), 1).astype(F32)
    ).astype(F32)
    gather = picks[:, :owned].astype(BF16)
    combine = picks.T[:owned].astype(BF16)
    combine = jnp.concatenate([combine, combine], axis=1)
    left = lax.broadcasted_iota(jnp.int32, (owned, 128), 1) < SHELLS
    for k in range(HALF + 1):
        high, low = split(parts[k * SLOTP : k * SLOTP + devices, :])
        both = dot(combine, jnp.concatenate([high, low], axis=0).astype(BF16))
        other = pltpu.roll(both, SHELLS, 1)
        at_k = (k if k < HALF else LM - 1) * owned
        acc[at_k : at_k + owned, :] = jnp.where(left, both, other)
        if k < HALF:
            at_k += HALF * owned
            acc[at_k : at_k + owned, :] = jnp.where(left, other, both)

    for d in range(LMAX + 1):
        begin, end = d * d, (d + 1) * (d + 1)
        twice = acc[begin * owned : end * owned, :]
        high, low = split(twice)
        wide = lax.broadcasted_iota(jnp.int32, twice.shape, 1) < SHELLS
        both = dot(jnp.where(wide, high, low).astype(BF16), green[d])
        thigh, tlow = split(both[:, :128] + both[:, 128:])
        small[begin * owned : end * owned, :] = jnp.where(wide, thigh, tlow).astype(BF16)
    for k in range(0, LM, 2):
        many = min(2, LM - k)
        rows = [small[n * owned : (n + 1) * owned, :] for n in range(k, k + many)]
        picked = dot(gather, jnp.concatenate(rows, axis=1))
        for n in range(many):
            at_k = (k + n) * SLOTP
            tables[at_k : at_k + devices, :] = picked[:, n * 128 : (n + 1) * 128]

    def evaluate(i):
        table = tables[pl.ds(i, KP, stride=SLOTP), :].astype(BF16)
        hot = hots[i]
        picked = dot(table, jnp.concatenate([hot, hot], axis=0))
        for h in range(2):
            y = ys[h, pl.ds(pl.multiple_of(i * KP, 8), KP), :]
            total = jnp.sum(
                picked[:, h * 128 : (h + 1) * 128] * y, axis=0, keepdims=True
            )
            reply[i, h : h + 1, :] = total

    def answer(begin, end):
        for i in range(max(begin, 1), end):
            pltpu.make_async_remote_copy(
                src_ref=reply.at[i],
                dst_ref=back.at[i],
                send_sem=reply_send,
                recv_sem=reply_recv,
                device_id=peer(i, -1),
                device_id_type=MESH,
            ).start()

    pairs = LM // 2
    for g in range(devices // WAVE):
        for i in range(g * WAVE, (g + 1) * WAVE):
            evaluate(i)
        for n in range(g * WAVE * pairs // devices, (g + 1) * WAVE * pairs // devices):
            first = acc[2 * n * owned : (2 * n + 1) * owned, :]
            second = acc[(2 * n + 1) * owned : (2 * n + 2) * owned, :]
            sums[:, n * 128 : (n + 1) * 128] = jnp.where(left, first, second)
        answer(g * WAVE, (g + 1) * WAVE)
    back[0] = reply[0]
    sums[:, pairs * 128 :] = acc[(LM - 1) * owned : LM * owned, :SHELLS]

    everything = pltpu.make_async_remote_copy(
        src_ref=piece(pay, 1, devices - 1),
        dst_ref=piece(arrived, 1, devices - 1),
        send_sem=send_sem,
        recv_sem=recv_sem.at[0],
        device_id=(0, 0),
        device_id_type=MESH,
    )
    everything.wait_send()
    answers = pltpu.make_async_remote_copy(
        src_ref=reply.at[pl.ds(1, devices - 1)],
        dst_ref=back.at[pl.ds(1, devices - 1)],
        send_sem=reply_send,
        recv_sem=reply_recv,
        device_id=(0, 0),
        device_id_type=MESH,
    )
    answers.wait_send()
    answers.wait_recv()


def finish_kernel(mine, back, sums, potential, moments, sem):
    whole = pltpu.make_async_copy(sums, moments, sem)
    whole.start()
    batches = potential.shape[0]
    chosen = mine[...].astype(BF16)
    for h in range(2):
        high, rest = split(back[:, h, :])
        middle, low = split(rest)
        total = (
            dot(chosen, high.astype(BF16))
            + dot(chosen, middle.astype(BF16))
            + dot(chosen, low.astype(BF16))
        )
        potential[:, h * 128 : (h + 1) * 128] = total[:batches]
    whole.wait()


VMEM = pl.BlockSpec(memory_space=pltpu.VMEM)
HBM = pl.BlockSpec(memory_space=pltpu.HBM)
SMEM = pl.BlockSpec(memory_space=pltpu.SMEM)


def body(
    point_coords,
    charge,
    shell_index,
    neighbours,
    neighbour_count,
    batch_load,
    atom_coords,
    owner_slot,
):
    batches, points = charge.shape
    slots = neighbours.shape[1]
    devices = lax.axis_size("gx") * lax.axis_size("gy")
    owned = owner_slot.shape[0] // devices
    spaces = batches * slots
    sds = jax.ShapeDtypeStruct
    green_table = green_blocks()
    sums, mine, back = pl.pallas_call(
        fused_kernel,
        out_shape=(
            sds((owned, LM * SHELLS), F32),
            sds((8, devices), F32),
            sds((devices, 2, 128), F32),
        ),
        in_specs=[SMEM] + [HBM] * 9,
        out_specs=(VMEM, VMEM, VMEM),
        scratch_shapes=[
            pltpu.SMEM((batches, slots), jnp.int32),
            pltpu.SMEM((batches,), jnp.int32),
            pltpu.SMEM(owner_slot.shape, jnp.int32),
            pltpu.SMEM(atom_coords.shape, F32),
            pltpu.VMEM((3, batches, points), F32),
            pltpu.VMEM((batches, points), F32),
            pltpu.VMEM((batches, slots, points), jnp.int32),
            pltpu.VMEM(green_table.shape, BF16),
            pltpu.VMEM((4, devices), jnp.int32),
            pltpu.VMEM((4, spaces, 128), F32),
            pltpu.VMEM((ROWS, spaces, 128), F32),
            pltpu.VMEM((devices, PITCH, 128), F32),
            pltpu.VMEM((devices, PITCH, 128), F32),
            pltpu.VMEM((2, devices * KP, 128), F32),
            pltpu.VMEM((2, devices, 128), F32),
            pltpu.VMEM((devices, SHELLS, 256), BF16),
            pltpu.VMEM(((HALF + 1) * SLOTP, 128), F32),
            pltpu.VMEM((LM * owned, 128), F32),
            pltpu.VMEM((LM * owned, 128), BF16),
            pltpu.VMEM((KP * SLOTP, 128), F32),
            pltpu.VMEM((devices, 2, 128), F32),
            pltpu.SemaphoreType.DMA((9,)),
            pltpu.SemaphoreType.DMA,
            pltpu.SemaphoreType.DMA((devices // WAVE,)),
            pltpu.SemaphoreType.DMA,
            pltpu.SemaphoreType.DMA,
        ],
        compiler_params=pltpu.CompilerParams(
            collective_id=0, has_side_effects=True, vmem_limit_bytes=34 << 20
        ),
        name="fused",
    )(
        batch_load,
        *[
            pltpu.with_memory_space_constraint(one, pltpu.HBM)
            for one in (
                neighbours,
                neighbour_count,
                owner_slot,
                atom_coords,
                jnp.transpose(point_coords, (1, 0, 2)),
                charge,
                shell_index,
                jnp.asarray(green_table),
                jnp.asarray(np.array(ORDER, dtype=np.int32).T),
            )
        ]
    )
    potential, moments = pl.pallas_call(
        finish_kernel,
        out_shape=(sds(charge.shape, F32), sds(sums.shape, F32)),
        in_specs=[VMEM] * 3,
        out_specs=(VMEM, HBM),
        scratch_shapes=[pltpu.SemaphoreType.DMA],
        compiler_params=pltpu.CompilerParams(vmem_limit_bytes=4 << 20),
        name="finish",
    )(mine, back, sums)
    return (potential, moments)


def solution(mesh):
    return jax.shard_map(
        body,
        mesh=mesh,
        in_specs=(
            P(("gx", "gy"), None, None),
            P(("gx", "gy"), None),
            P(("gx", "gy"), None, None),
            P(("gx", "gy"), None),
            P(("gx", "gy")),
            P(("gx", "gy")),
            P(),
            P(),
        ),
        out_specs=(P(("gx", "gy"), None), P(("gx", "gy"), None)),
        check_vma=False,
    )
```

```python
import math

import jax
import jax.numpy as jnp
import numpy as np
from jax import lax
from jax.experimental import pallas as pl
from jax.experimental.pallas import tpu as pltpu
from jax.sharding import PartitionSpec as P

LOGICAL = pl.DeviceIdType.LOGICAL
F32 = jnp.float32
BF16 = jnp.bfloat16
SHELLS = 64
LMAX = 6
LM = 49
KP = 56
HALF = 24
LANES = 8
SOFTEN = 0.01
ROWS = 10
PITCH = 16
SLOTP = 136
WAVE = 32


def green_blocks():
    rank = np.arange(SHELLS, dtype=np.float64)
    radius = 0.5 * np.exp(2.3 * rank / SHELLS)
    nearer = np.minimum(radius[:, None], radius[None, :])
    farther = np.maximum(radius[:, None], radius[None, :])
    full = np.stack(
        [
            4.0 * math.pi / (2 * d + 1) * nearer**d / farther ** (d + 1)
            for d in range(LMAX + 1)
        ]
    )
    full = np.concatenate([full, full], axis=2).astype(np.float32)
    high = full.astype(jnp.bfloat16)
    low = (full - high.astype(np.float32)).astype(jnp.bfloat16)
    upper = np.concatenate([high, low], axis=2)
    lower = np.concatenate([high, np.zeros_like(low)], axis=2)
    return np.concatenate([upper, lower], axis=1)


def split(x):
    high = x.astype(BF16).astype(F32)
    return high, x - high


def dot(a, b, dims=((1,), (0,))):
    return lax.dot_general(a, b, (dims, ((), ())), preferred_element_type=F32)


def harmonics(ux, uy, uz):
    cosine = [None]
    sine = [None]
    for m in range(1, LMAX + 1):
        if m == 1:
            cosine.append(ux)
            sine.append(uy)
        else:
            pc, ps = cosine[-1], sine[-1]
            cosine.append(pc * ux - ps * uy)
            sine.append(pc * uy + ps * ux)

    def norm(d, m):
        value = math.sqrt(
            (2 * d + 1) / (4 * math.pi) * math.factorial(d - m) / math.factorial(d + m)
        )
        return value * (math.sqrt(2.0) if m else 1.0)

    out = {}
    for m in range(LMAX + 1):
        start = norm(m, m) * float(math.prod(range(1, 2 * m, 2)))
        older, old = None, None
        for d in range(m, LMAX + 1):
            if d == m:
                now = start
            elif d == m + 1:
                now = uz * ((2 * m + 1) * start * norm(d, m) / norm(m, m))
            else:
                ca = (2 * d - 1) / (d - m) * norm(d, m) / norm(d - 1, m)
                cb = (d + m - 1) / (d - m) * norm(d, m) / norm(d - 2, m)
                now = (ca * uz) * old - cb * older
            if m == 0:
                out[d * d + d] = now if d else jnp.full(ux.shape, start, F32)
            else:
                out[d * d + d + m] = cosine[m] * now
                out[d * d + d - m] = sine[m] * now
            older, old = old, now
    return out


def visiting_order():
    every = [
        (dy, dz, dx, dc)
        for dy in range(4)
        for dz in range(4)
        for dx in range(4)
        for dc in range(2)
    ]

    def far(t):
        return sum(min(v, 4 - v) for v in t[:3])

    return every[:1] + sorted(every[1:], key=far, reverse=True)


ORDER = visiting_order()


def fused_kernel(
    *refs,
):
    load, given, refs = refs[0], refs[1:10], refs[10:]
    sums, mine, back = refs[:3]
    held, refs = refs[3:12], refs[12:]
    (
        place,
        src,
        pay,
        arrived,
        ys,
        ws,
        hots,
        parts,
        acc,
        small,
        tables,
        reply,
        names,
        called,
        load_sem,
        send_sem,
        recv_sem,
        reply_send,
        reply_recv,
        name_send,
        name_recv,
    ) = refs
    labels, count, owner, atoms, coords, charge, shell, green, steps = held
    loads = [
        pltpu.make_async_copy(given[n], held[n], load_sem.at[n])
        for n in range(len(held))
    ]
    for one in loads:
        one.start()
    batches, slots = labels.shape
    spaces = batches * slots
    devices = pay.shape[0]
    owned = sums.shape[0]
    gy = lax.axis_index("gy")
    at = (lax.axis_index("gx"), gy // 8, lax.rem(gy, 8) // 2, lax.rem(gy, 2))
    spans, scales = (4, 4, 4, 2), (32, 8, 2, 1)
    moved_to = [
        [lax.rem(at[axis] + step, spans[axis]) * scales[axis] for step in range(spans[axis])]
        for axis in range(4)
    ]
    planes = {
        (dy, dz): moved_to[0][dy] + moved_to[1][dz] for dy in range(4) for dz in range(4)
    }
    lines = {
        (dx, dc): moved_to[2][dx] + moved_to[3][dc] for dx in range(4) for dc in range(2)
    }

    def peer(i, sign):
        dy, dz, dx, dc = [sign * d % span for d, span in zip(ORDER[i], spans)]
        return planes[dy, dz] + lines[dx, dc]

    barrier = pltpu.get_barrier_semaphore()
    for i in range(1, devices):
        pl.semaphore_signal(
            barrier, inc=1, device_id=peer(i, -1), device_id_type=LOGICAL
        )

    top = jnp.where(
        lax.broadcasted_iota(jnp.int32, (8, 128), 0) == 0,
        math.sqrt(1 / (4 * math.pi)),
        0.0,
    ).astype(F32)

    @pl.loop(0, devices)
    def _(i):
        for h in range(2):
            ys[h, pl.ds(pl.multiple_of(i * KP, 8), 8), :] = top
            ys[h, pl.ds(pl.multiple_of(i * KP + KP - 8, 8), 8), :] = jnp.zeros_like(top)

    for k in range(LM, KP):
        tables[k * SLOTP : k * SLOTP + devices, :] = jnp.zeros((devices, 128), F32)
    parts[(HALF * SLOTP) :, :] = jnp.zeros((SLOTP, 128), F32)

    for one in loads:
        one.wait()
    for b in range(batches):

        @pl.loop(0, slots, unroll=4)
        def _(s):
            label = labels[b, s]
            target = owner[label]
            row = b * slots + s
            for c in range(3):
                place[c, pl.ds(row, 1), :] = jnp.full((1, 128), atoms[c, label], F32)
            place[3, pl.ds(row, 1), :] = jnp.full(
                (1, 128), (target // owned).astype(F32), F32
            )
            src[10, pl.ds(row, 1), :] = jnp.full(
                (1, 128), lax.rem(target, owned).astype(F32), F32
            )

    slot_rank = lax.broadcasted_iota(jnp.int32, (slots, 128), 0)
    lane = lax.broadcasted_iota(jnp.int32, (slots, 128), 1)
    lives = []
    for b in range(batches):
        live = jnp.clip(load[0] - b, 0, 1).astype(F32)
        slot_live = jnp.clip(count[b] - slot_rank, 0, 1).astype(F32)
        here = slice(b * slots, (b + 1) * slots)
        lives.append(jnp.where(lane == b, slot_live * live, 0.0))
        for h in range(2):
            points = slice(h * 128, (h + 1) * 128)
            squared = 0.0
            for c in range(3):
                offset = coords[c, b : b + 1, points] - place[c, here, :]
                src[2 * c + h, here, :] = offset
                squared = squared + offset * offset
            closeness = slot_live / (1.0 + squared)
            total = jnp.sum(closeness, axis=0, keepdims=True)
            scaled = charge[b : b + 1, points] * live / total
            src[6 + h, here, :] = shell[b, :, points].astype(F32)
            src[8 + h, here, :] = slot_live * scaled

    row_of = 0
    for axis in range(4):
        there = lax.rem(steps[axis : axis + 1, :] + at[axis], spans[axis])
        row_of = row_of * spans[axis] + there
    goes = (place[3] == row_of.astype(F32)).astype(F32)
    goes = goes.T.astype(BF16)
    flat_pay = pay.reshape(devices * PITCH, 128)
    for r in range(ROWS + 1):
        high, rest = split(src[r])
        moved = dot(goes, high.astype(BF16))
        if r not in (6, 7, 10):
            middle, low = split(rest)
            moved = (
                moved + dot(goes, middle.astype(BF16)) + dot(goes, low.astype(BF16))
            )
        if r < ROWS:
            flat_pay[pl.ds(r, devices, stride=PITCH), :] = moved
        else:
            names[...] = moved[:, :LANES]
    lives = dot(goes, jnp.concatenate(lives, axis=0).astype(BF16))
    mine[...] = lives.T[:8]

    pl.semaphore_wait(barrier, devices - 1)

    def piece(ref, i, size=1):
        return ref.at[pl.ds(i, size), pl.ds(0, ROWS)]

    for i in range(1, devices):
        pltpu.make_async_remote_copy(
            src_ref=piece(pay, i),
            dst_ref=piece(arrived, i),
            send_sem=send_sem,
            recv_sem=recv_sem.at[i // WAVE],
            device_id=peer(i, 1),
            device_id_type=LOGICAL,
        ).start()

    def called_by(i, size):
        return names.at[pl.ds(i, size)], called.at[pl.ds(i, size)]

    for i in range(1, devices):
        here_name, there_name = called_by(i, 1)
        pltpu.make_async_remote_copy(
            src_ref=here_name,
            dst_ref=there_name,
            send_sem=name_send,
            recv_sem=name_recv,
            device_id=peer(i, 1),
            device_id_type=LOGICAL,
        ).start()
    called[0:1, :] = names[0:1, :]
    arrived[0] = pay[0]
    flat = arrived.reshape(devices * PITCH, 128)
    shell_rank = lax.broadcasted_iota(jnp.int32, (SHELLS, 128), 0).astype(F32)

    def shapes(g):
        for h in range(2):

            def row(r):
                return flat[pl.ds(g * 8 * PITCH + 2 * r + h, 8, stride=PITCH), :]

            dx, dy, dz = row(0), row(1), row(2)
            squared = dx * dx + dy * dy + dz * dz
            scale = lax.rsqrt(squared + SOFTEN)
            ws[h, pl.ds(pl.multiple_of(g * 8, 8), 8), :] = row(4) / (1.0 + squared)
            values = harmonics(dx * scale, dy * scale, dz * scale)
            for k in range(1, LM):
                ys[h, pl.ds(g * 8 * KP + k, 8, stride=KP), :] = values[k]

    def forward(i):
        stack, hot = [], []
        for h in range(2):
            y = ys[h, pl.ds(pl.multiple_of(i * KP, 8), KP), :]
            weighted = y * ws[h, pl.ds(i, 1), :]
            high, low = split(weighted)
            stack.append(jnp.concatenate([high, low], axis=0).astype(BF16))
            shells = flat[pl.ds(i * PITCH + 6 + h, 1), :]
            hot.append((shells == shell_rank).astype(F32).astype(BF16))
        hot = jnp.concatenate(hot, axis=1)
        hots[i] = hot
        both = dot(jnp.concatenate(stack, axis=1), hot, ((1,), (1,)))
        part = both[:KP] + both[KP:]
        parts[pl.ds(i, HALF, stride=SLOTP), :] = jnp.concatenate(
            [part[:HALF], part[HALF : 2 * HALF]], axis=1
        )
        parts[pl.ds(HALF * SLOTP + i, 1), :SHELLS] = part[2 * HALF : LM]

    def landed(g, size):
        pltpu.make_async_remote_copy(
            src_ref=piece(pay, 1, size),
            dst_ref=piece(arrived, 1, size),
            send_sem=send_sem,
            recv_sem=recv_sem.at[g],
            device_id=0,
            device_id_type=LOGICAL,
        ).wait_recv()

    @pl.loop(0, devices // WAVE)
    def _(g):
        @pl.when(g == 0)
        def _():
            landed(g, WAVE - 1)

        @pl.when(g > 0)
        def _():
            landed(g, WAVE)

        for q in range(WAVE // 8):
            shapes(g * (WAVE // 8) + q)

        for e in range(WAVE):
            forward(g * WAVE + e)

    here_names, there_names = called_by(1, devices - 1)
    called_all = pltpu.make_async_remote_copy(
        src_ref=here_names,
        dst_ref=there_names,
        send_sem=name_send,
        recv_sem=name_recv,
        device_id=0,
        device_id_type=LOGICAL,
    )
    called_all.wait_send()
    called_all.wait_recv()
    marks = jnp.broadcast_to(called[:, :1], (devices, 128))
    picks = (
        marks == lax.broadcasted_iota(jnp.int32, (devices, 128), 1).astype(F32)
    ).astype(F32)
    gather = picks[:, :owned].astype(BF16)
    combine = picks.T[:owned].astype(BF16)
    combine = jnp.concatenate([combine, combine], axis=1)
    left = lax.broadcasted_iota(jnp.int32, (owned, 128), 1) < SHELLS
    for k in range(HALF + 1):
        high, low = split(parts[k * SLOTP : k * SLOTP + devices, :])
        both = dot(combine, jnp.concatenate([high, low], axis=0).astype(BF16))
        other = pltpu.roll(both, SHELLS, 1)
        at_k = (k if k < HALF else LM - 1) * owned
        acc[at_k : at_k + owned, :] = jnp.where(left, both, other)
        if k < HALF:
            at_k += HALF * owned
            acc[at_k : at_k + owned, :] = jnp.where(left, other, both)

    for d in range(LMAX + 1):
        begin, end = d * d, (d + 1) * (d + 1)
        twice = acc[begin * owned : end * owned, :]
        high, low = split(twice)
        wide = lax.broadcasted_iota(jnp.int32, twice.shape, 1) < SHELLS
        both = dot(jnp.where(wide, high, low).astype(BF16), green[d])
        thigh, tlow = split(both[:, :128] + both[:, 128:])
        small[begin * owned : end * owned, :] = jnp.where(wide, thigh, tlow).astype(BF16)
    for k in range(0, LM, 2):
        many = min(2, LM - k)
        rows = [small[n * owned : (n + 1) * owned, :] for n in range(k, k + many)]
        picked = dot(gather, jnp.concatenate(rows, axis=1))
        for n in range(many):
            at_k = (k + n) * SLOTP
            tables[at_k : at_k + devices, :] = picked[:, n * 128 : (n + 1) * 128]

    def evaluate(i):
        table = tables[pl.ds(i, KP, stride=SLOTP), :].astype(BF16)
        hot = hots[i]
        picked = dot(table, jnp.concatenate([hot, hot], axis=0))
        for h in range(2):
            y = ys[h, pl.ds(pl.multiple_of(i * KP, 8), KP), :]
            total = jnp.sum(
                picked[:, h * 128 : (h + 1) * 128] * y, axis=0, keepdims=True
            )
            reply[i, h : h + 1, :] = total

    def answer(begin, end):
        for i in range(max(begin, 1), end):
            pltpu.make_async_remote_copy(
                src_ref=reply.at[i],
                dst_ref=back.at[i],
                send_sem=reply_send,
                recv_sem=reply_recv,
                device_id=peer(i, -1),
                device_id_type=LOGICAL,
            ).start()

    pairs = LM // 2
    for g in range(devices // WAVE):
        for i in range(g * WAVE, (g + 1) * WAVE):
            evaluate(i)
        for n in range(g * WAVE * pairs // devices, (g + 1) * WAVE * pairs // devices):
            first = acc[2 * n * owned : (2 * n + 1) * owned, :]
            second = acc[(2 * n + 1) * owned : (2 * n + 2) * owned, :]
            sums[:, n * 128 : (n + 1) * 128] = jnp.where(left, first, second)
        answer(g * WAVE, (g + 1) * WAVE)
    back[0] = reply[0]
    sums[:, pairs * 128 :] = acc[(LM - 1) * owned : LM * owned, :SHELLS]

    everything = pltpu.make_async_remote_copy(
        src_ref=piece(pay, 1, devices - 1),
        dst_ref=piece(arrived, 1, devices - 1),
        send_sem=send_sem,
        recv_sem=recv_sem.at[0],
        device_id=0,
        device_id_type=LOGICAL,
    )
    everything.wait_send()
    answers = pltpu.make_async_remote_copy(
        src_ref=reply.at[pl.ds(1, devices - 1)],
        dst_ref=back.at[pl.ds(1, devices - 1)],
        send_sem=reply_send,
        recv_sem=reply_recv,
        device_id=0,
        device_id_type=LOGICAL,
    )
    answers.wait_send()
    answers.wait_recv()


def finish_kernel(mine, back, sums, potential, moments, sem):
    whole = pltpu.make_async_copy(sums, moments, sem)
    whole.start()
    batches = potential.shape[0]
    chosen = mine[...].astype(BF16)
    for h in range(2):
        high, rest = split(back[:, h, :])
        middle, low = split(rest)
        total = (
            dot(chosen, high.astype(BF16))
            + dot(chosen, middle.astype(BF16))
            + dot(chosen, low.astype(BF16))
        )
        potential[:, h * 128 : (h + 1) * 128] = total[:batches]
    whole.wait()


VMEM = pl.BlockSpec(memory_space=pltpu.VMEM)
HBM = pl.BlockSpec(memory_space=pltpu.HBM)
SMEM = pl.BlockSpec(memory_space=pltpu.SMEM)


def body(
    point_coords,
    charge,
    shell_index,
    neighbours,
    neighbour_count,
    batch_load,
    atom_coords,
    owner_slot,
):
    batches, points = charge.shape
    slots = neighbours.shape[1]
    devices = lax.axis_size("gx") * lax.axis_size("gy")
    owned = owner_slot.shape[0] // devices
    spaces = batches * slots
    sds = jax.ShapeDtypeStruct
    green_table = green_blocks()
    sums, mine, back = pl.pallas_call(
        fused_kernel,
        out_shape=(
            sds((owned, LM * SHELLS), F32),
            sds((8, devices), F32),
            sds((devices, 2, 128), F32),
        ),
        in_specs=[SMEM] + [HBM] * 9,
        out_specs=(VMEM, VMEM, VMEM),
        scratch_shapes=[
            pltpu.SMEM((batches, slots), jnp.int32),
            pltpu.SMEM((batches,), jnp.int32),
            pltpu.SMEM(owner_slot.shape, jnp.int32),
            pltpu.SMEM(atom_coords.shape, F32),
            pltpu.VMEM((3, batches, points), F32),
            pltpu.VMEM((batches, points), F32),
            pltpu.VMEM((batches, slots, points), jnp.int32),
            pltpu.VMEM(green_table.shape, BF16),
            pltpu.VMEM((4, devices), jnp.int32),
            pltpu.VMEM((4, spaces, 128), F32),
            pltpu.VMEM((ROWS + 1, spaces, 128), F32),
            pltpu.VMEM((devices, PITCH, 128), F32),
            pltpu.VMEM((devices, PITCH, 128), F32),
            pltpu.VMEM((2, devices * KP, 128), F32),
            pltpu.VMEM((2, devices, 128), F32),
            pltpu.VMEM((devices, SHELLS, 256), BF16),
            pltpu.VMEM(((HALF + 1) * SLOTP, 128), F32),
            pltpu.VMEM((LM * owned, 128), F32),
            pltpu.VMEM((LM * owned, 128), BF16),
            pltpu.VMEM((KP * SLOTP, 128), F32),
            pltpu.VMEM((devices, 2, 128), F32),
            pltpu.VMEM((devices, LANES), F32),
            pltpu.VMEM((devices, LANES), F32),
            pltpu.SemaphoreType.DMA((9,)),
            pltpu.SemaphoreType.DMA,
            pltpu.SemaphoreType.DMA((devices // WAVE,)),
            pltpu.SemaphoreType.DMA,
            pltpu.SemaphoreType.DMA,
            pltpu.SemaphoreType.DMA,
            pltpu.SemaphoreType.DMA,
        ],
        compiler_params=pltpu.CompilerParams(
            collective_id=0, has_side_effects=True, vmem_limit_bytes=34 << 20
        ),
        name="fused",
    )(
        batch_load,
        *[
            pltpu.with_memory_space_constraint(one, pltpu.HBM)
            for one in (
                neighbours,
                neighbour_count,
                owner_slot,
                atom_coords,
                jnp.transpose(point_coords, (1, 0, 2)),
                charge,
                shell_index,
                jnp.asarray(green_table),
                jnp.asarray(np.array(ORDER, dtype=np.int32).T),
            )
        ]
    )
    potential, moments = pl.pallas_call(
        finish_kernel,
        out_shape=(sds(charge.shape, F32), sds(sums.shape, F32)),
        in_specs=[VMEM] * 3,
        out_specs=(VMEM, HBM),
        scratch_shapes=[pltpu.SemaphoreType.DMA],
        compiler_params=pltpu.CompilerParams(vmem_limit_bytes=4 << 20),
        name="finish",
    )(mine, back, sums)
    return (potential, moments)


def solution(mesh):
    return jax.shard_map(
        body,
        mesh=mesh,
        in_specs=(
            P(("gx", "gy"), None, None),
            P(("gx", "gy"), None),
            P(("gx", "gy"), None, None),
            P(("gx", "gy"), None),
            P(("gx", "gy")),
            P(("gx", "gy")),
            P(),
            P(),
        ),
        out_specs=(P(("gx", "gy"), None), P(("gx", "gy"), None)),
        check_vma=False,
    )
```

```python
import math

import jax
import jax.numpy as jnp
import numpy as np
from jax import lax
from jax.experimental import pallas as pl
from jax.experimental.pallas import tpu as pltpu
from jax.sharding import PartitionSpec as P

LOGICAL = pl.DeviceIdType.LOGICAL
F32 = jnp.float32
BF16 = jnp.bfloat16
SHELLS = 64
LMAX = 6
LM = 49
KP = 56
HALF = 24
LANES = 8
SOFTEN = 0.01
ROWS = 10
PITCH = 16
SLOTP = 136
WAVE = 32


def green_blocks():
    rank = np.arange(SHELLS, dtype=np.float64)
    radius = 0.5 * np.exp(2.3 * rank / SHELLS)
    nearer = np.minimum(radius[:, None], radius[None, :])
    farther = np.maximum(radius[:, None], radius[None, :])
    full = np.stack(
        [
            4.0 * math.pi / (2 * d + 1) * nearer**d / farther ** (d + 1)
            for d in range(LMAX + 1)
        ]
    )
    full = np.concatenate([full, full], axis=2).astype(np.float32)
    high = full.astype(jnp.bfloat16)
    low = (full - high.astype(np.float32)).astype(jnp.bfloat16)
    upper = np.concatenate([high, low], axis=2)
    lower = np.concatenate([high, np.zeros_like(low)], axis=2)
    return np.concatenate([upper, lower], axis=1)


def split(x):
    high = x.astype(BF16).astype(F32)
    return high, x - high


def dot(a, b, dims=((1,), (0,))):
    return lax.dot_general(a, b, (dims, ((), ())), preferred_element_type=F32)


def harmonics(ux, uy, uz):
    cosine = [None]
    sine = [None]
    for m in range(1, LMAX + 1):
        if m == 1:
            cosine.append(ux)
            sine.append(uy)
        else:
            pc, ps = cosine[-1], sine[-1]
            cosine.append(pc * ux - ps * uy)
            sine.append(pc * uy + ps * ux)

    def norm(d, m):
        value = math.sqrt(
            (2 * d + 1) / (4 * math.pi) * math.factorial(d - m) / math.factorial(d + m)
        )
        return value * (math.sqrt(2.0) if m else 1.0)

    out = {}
    for m in range(LMAX + 1):
        start = norm(m, m) * float(math.prod(range(1, 2 * m, 2)))
        older, old = None, None
        for d in range(m, LMAX + 1):
            if d == m:
                now = start
            elif d == m + 1:
                now = uz * ((2 * m + 1) * start * norm(d, m) / norm(m, m))
            else:
                ca = (2 * d - 1) / (d - m) * norm(d, m) / norm(d - 1, m)
                cb = (d + m - 1) / (d - m) * norm(d, m) / norm(d - 2, m)
                now = (ca * uz) * old - cb * older
            if m == 0:
                out[d * d + d] = now if d else jnp.full(ux.shape, start, F32)
            else:
                out[d * d + d + m] = cosine[m] * now
                out[d * d + d - m] = sine[m] * now
            older, old = old, now
    return out


def visiting_order():
    every = [
        (dy, dz, dx, dc)
        for dy in range(4)
        for dz in range(4)
        for dx in range(4)
        for dc in range(2)
    ]

    def far(t):
        return sum(min(v, 4 - v) for v in t[:3])

    return every[:1] + sorted(every[1:], key=far, reverse=True)


ORDER = visiting_order()


def fused_kernel(
    *refs,
):
    load, given, refs = refs[0], refs[1:10], refs[10:]
    sums, mine, back = refs[:3]
    held, refs = refs[3:12], refs[12:]
    (
        place,
        src,
        pay,
        arrived,
        ys,
        ws,
        hots,
        parts,
        acc,
        small,
        tables,
        reply,
        names,
        called,
        load_sem,
        send_sem,
        recv_sem,
        reply_send,
        reply_recv,
        name_send,
        name_recv,
    ) = refs
    labels, count, owner, atoms, coords, charge, shell, green, steps = held
    loads = [
        pltpu.make_async_copy(given[n], held[n], load_sem.at[n])
        for n in range(len(held))
    ]
    for one in loads:
        one.start()
    batches, slots = labels.shape
    spaces = batches * slots
    devices = back.shape[0]
    owned = sums.shape[0]
    gy = lax.axis_index("gy")
    at = (lax.axis_index("gx"), gy // 8, lax.rem(gy, 8) // 2, lax.rem(gy, 2))
    spans, scales = (4, 4, 4, 2), (32, 8, 2, 1)
    moved_to = [
        [lax.rem(at[axis] + step, spans[axis]) * scales[axis] for step in range(spans[axis])]
        for axis in range(4)
    ]
    planes = {
        (dy, dz): moved_to[0][dy] + moved_to[1][dz] for dy in range(4) for dz in range(4)
    }
    lines = {
        (dx, dc): moved_to[2][dx] + moved_to[3][dc] for dx in range(4) for dc in range(2)
    }

    def peer(i, sign):
        dy, dz, dx, dc = [sign * d % span for d, span in zip(ORDER[i], spans)]
        return planes[dy, dz] + lines[dx, dc]

    barrier = pltpu.get_barrier_semaphore()
    for i in range(1, devices):
        pl.semaphore_signal(
            barrier, inc=1, device_id=peer(i, -1), device_id_type=LOGICAL
        )

    top = jnp.where(
        lax.broadcasted_iota(jnp.int32, (8, 128), 0) == 0,
        math.sqrt(1 / (4 * math.pi)),
        0.0,
    ).astype(F32)

    @pl.loop(0, devices)
    def _(i):
        for h in range(2):
            ys[h, pl.ds(pl.multiple_of(i * KP, 8), 8), :] = top
            ys[h, pl.ds(pl.multiple_of(i * KP + KP - 8, 8), 8), :] = jnp.zeros_like(top)

    for k in range(LM, KP):
        tables[k * SLOTP : k * SLOTP + devices, :] = jnp.zeros((devices, 128), F32)
    parts[HALF * SLOTP : (HALF + 1) * SLOTP, :] = jnp.zeros((SLOTP, 128), F32)

    for one in loads:
        one.wait()
    for b in range(batches):

        @pl.loop(0, slots, unroll=4)
        def _(s):
            label = labels[b, s]
            target = owner[label]
            row = b * slots + s
            for c in range(3):
                place[c, pl.ds(row, 1), :] = jnp.full((1, 128), atoms[c, label], F32)
            place[3, pl.ds(row, 1), :] = jnp.full(
                (1, 128), (target // owned).astype(F32), F32
            )
            src[10, pl.ds(row, 1), :] = jnp.full(
                (1, 128), lax.rem(target, owned).astype(F32), F32
            )

    slot_rank = lax.broadcasted_iota(jnp.int32, (slots, 128), 0)
    lane = lax.broadcasted_iota(jnp.int32, (slots, 128), 1)
    lives = []
    for b in range(batches):
        live = jnp.clip(load[0] - b, 0, 1).astype(F32)
        slot_live = jnp.clip(count[b] - slot_rank, 0, 1).astype(F32)
        here = slice(b * slots, (b + 1) * slots)
        lives.append(jnp.where(lane == b, slot_live * live, 0.0))
        for h in range(2):
            points = slice(h * 128, (h + 1) * 128)
            squared = 0.0
            for c in range(3):
                offset = coords[c, b : b + 1, points] - place[c, here, :]
                src[2 * c + h, here, :] = offset
                squared = squared + offset * offset
            closeness = slot_live / (1.0 + squared)
            total = jnp.sum(closeness, axis=0, keepdims=True)
            scaled = charge[b : b + 1, points] * live / total
            src[6 + h, here, :] = shell[b, :, points].astype(F32)
            src[8 + h, here, :] = slot_live * scaled

    row_of = 0
    for axis in range(4):
        there = lax.rem(steps[axis : axis + 1, :] + at[axis], spans[axis])
        row_of = row_of * spans[axis] + there
    goes = (place[3, :spaces] == row_of.astype(F32)).astype(F32)
    goes = goes.T.astype(BF16)
    flat_pay = pay.reshape((devices + 1) * PITCH, 128)
    for r in range(ROWS + 1):
        high, rest = split(src[r, :spaces])
        moved = dot(goes, high.astype(BF16))
        if r not in (6, 7, 10):
            middle, low = split(rest)
            moved = (
                moved + dot(goes, middle.astype(BF16)) + dot(goes, low.astype(BF16))
            )
        if r < ROWS:
            flat_pay[pl.ds(r, devices, stride=PITCH), :] = moved
        else:
            names[...] = moved[:, :LANES]
    lives = dot(goes, jnp.concatenate(lives, axis=0).astype(BF16))
    mine[...] = lives.T[:8]

    pl.semaphore_wait(barrier, devices - 1)

    def piece(ref, i, size=1):
        return ref.at[pl.ds(i, size), pl.ds(0, ROWS)]

    for i in range(1, devices):
        pltpu.make_async_remote_copy(
            src_ref=piece(pay, i),
            dst_ref=piece(arrived, i),
            send_sem=send_sem,
            recv_sem=recv_sem.at[i // WAVE],
            device_id=peer(i, 1),
            device_id_type=LOGICAL,
        ).start()

    def called_by(i, size):
        return names.at[pl.ds(i, size)], called.at[pl.ds(i, size)]

    for i in range(1, devices):
        here_name, there_name = called_by(i, 1)
        pltpu.make_async_remote_copy(
            src_ref=here_name,
            dst_ref=there_name,
            send_sem=name_send,
            recv_sem=name_recv,
            device_id=peer(i, 1),
            device_id_type=LOGICAL,
        ).start()
    called[0:1, :] = names[0:1, :]
    arrived[0] = pay[0]
    flat = arrived.reshape((devices + 1) * PITCH, 128)
    shell_rank = lax.broadcasted_iota(jnp.int32, (SHELLS, 128), 0).astype(F32)

    def shapes(g):
        for h in range(2):

            def row(r):
                return flat[pl.ds(g * 8 * PITCH + 2 * r + h, 8, stride=PITCH), :]

            dx, dy, dz = row(0), row(1), row(2)
            squared = dx * dx + dy * dy + dz * dz
            scale = lax.rsqrt(squared + SOFTEN)
            ws[h, pl.ds(pl.multiple_of(g * 8, 8), 8), :] = row(4) / (1.0 + squared)
            values = harmonics(dx * scale, dy * scale, dz * scale)
            for k in range(1, LM):
                ys[h, pl.ds(g * 8 * KP + k, 8, stride=KP), :] = values[k]

    def forward(i):
        stack, hot = [], []
        for h in range(2):
            y = ys[h, pl.ds(pl.multiple_of(i * KP, 8), KP), :]
            weighted = y * ws[h, pl.ds(i, 1), :]
            high, low = split(weighted)
            stack.append(jnp.concatenate([high, low], axis=0).astype(BF16))
            shells = flat[pl.ds(i * PITCH + 6 + h, 1), :]
            hot.append((shells == shell_rank).astype(F32).astype(BF16))
        hot = jnp.concatenate(hot, axis=1)
        hots[i] = hot
        both = dot(jnp.concatenate(stack, axis=1), hot, ((1,), (1,)))
        part = both[:KP] + both[KP:]
        parts[pl.ds(i, HALF, stride=SLOTP), :] = jnp.concatenate(
            [part[:HALF], part[HALF : 2 * HALF]], axis=1
        )
        parts[pl.ds(HALF * SLOTP + i, 1), :SHELLS] = part[2 * HALF : LM]

    def landed(g, size):
        pltpu.make_async_remote_copy(
            src_ref=piece(pay, 1, size),
            dst_ref=piece(arrived, 1, size),
            send_sem=send_sem,
            recv_sem=recv_sem.at[g],
            device_id=0,
            device_id_type=LOGICAL,
        ).wait_recv()

    @pl.loop(0, devices // WAVE)
    def _(g):
        @pl.when(g == 0)
        def _():
            landed(g, WAVE - 1)

        @pl.when(g > 0)
        def _():
            landed(g, WAVE)

        for q in range(WAVE // 8):
            shapes(g * (WAVE // 8) + q)

        for e in range(WAVE):
            forward(g * WAVE + e)

    here_names, there_names = called_by(1, devices - 1)
    called_all = pltpu.make_async_remote_copy(
        src_ref=here_names,
        dst_ref=there_names,
        send_sem=name_send,
        recv_sem=name_recv,
        device_id=0,
        device_id_type=LOGICAL,
    )
    called_all.wait_send()
    called_all.wait_recv()
    marks = jnp.broadcast_to(called[:, :1], (devices, 128))
    picks = (
        marks == lax.broadcasted_iota(jnp.int32, (devices, 128), 1).astype(F32)
    ).astype(F32)
    gather = picks[:, :owned].astype(BF16)
    combine = picks.T[:owned].astype(BF16)
    combine = jnp.concatenate([combine, combine], axis=1)
    left = lax.broadcasted_iota(jnp.int32, (owned, 128), 1) < SHELLS
    for k in range(HALF + 1):
        high, low = split(parts[k * SLOTP : k * SLOTP + devices, :])
        both = dot(combine, jnp.concatenate([high, low], axis=0).astype(BF16))
        other = pltpu.roll(both, SHELLS, 1)
        at_k = (k if k < HALF else LM - 1) * owned
        acc[at_k : at_k + owned, :] = jnp.where(left, both, other)
        if k < HALF:
            at_k += HALF * owned
            acc[at_k : at_k + owned, :] = jnp.where(left, other, both)

    for d in range(LMAX + 1):
        begin, end = d * d, (d + 1) * (d + 1)
        twice = acc[begin * owned : end * owned, :]
        high, low = split(twice)
        wide = lax.broadcasted_iota(jnp.int32, twice.shape, 1) < SHELLS
        both = dot(jnp.where(wide, high, low).astype(BF16), green[d])
        thigh, tlow = split(both[:, :128] + both[:, 128:])
        small[begin * owned : end * owned, :] = jnp.where(wide, thigh, tlow).astype(BF16)
    for k in range(0, LM, 2):
        many = min(2, LM - k)
        rows = [small[n * owned : (n + 1) * owned, :] for n in range(k, k + many)]
        picked = dot(gather, jnp.concatenate(rows, axis=1))
        for n in range(many):
            at_k = (k + n) * SLOTP
            tables[at_k : at_k + devices, :] = picked[:, n * 128 : (n + 1) * 128]

    def evaluate(i):
        table = tables[pl.ds(i, KP, stride=SLOTP), :].astype(BF16)
        hot = hots[i]
        picked = dot(table, jnp.concatenate([hot, hot], axis=0))
        for h in range(2):
            y = ys[h, pl.ds(pl.multiple_of(i * KP, 8), KP), :]
            total = jnp.sum(
                picked[:, h * 128 : (h + 1) * 128] * y, axis=0, keepdims=True
            )
            reply[i, h : h + 1, :] = total

    def answer(begin, end):
        for i in range(max(begin, 1), end):
            pltpu.make_async_remote_copy(
                src_ref=reply.at[i],
                dst_ref=back.at[i],
                send_sem=reply_send,
                recv_sem=reply_recv,
                device_id=peer(i, -1),
                device_id_type=LOGICAL,
            ).start()

    pairs = LM // 2
    for g in range(devices // WAVE):
        for i in range(g * WAVE, (g + 1) * WAVE):
            evaluate(i)
        for n in range(g * WAVE * pairs // devices, (g + 1) * WAVE * pairs // devices):
            first = acc[2 * n * owned : (2 * n + 1) * owned, :]
            second = acc[(2 * n + 1) * owned : (2 * n + 2) * owned, :]
            sums[:, n * 128 : (n + 1) * 128] = jnp.where(left, first, second)
        answer(g * WAVE, (g + 1) * WAVE)
    back[0] = reply[0]
    sums[:, pairs * 128 :] = acc[(LM - 1) * owned : LM * owned, :SHELLS]

    everything = pltpu.make_async_remote_copy(
        src_ref=piece(pay, 1, devices - 1),
        dst_ref=piece(arrived, 1, devices - 1),
        send_sem=send_sem,
        recv_sem=recv_sem.at[0],
        device_id=0,
        device_id_type=LOGICAL,
    )
    everything.wait_send()
    answers = pltpu.make_async_remote_copy(
        src_ref=reply.at[pl.ds(1, devices - 1)],
        dst_ref=back.at[pl.ds(1, devices - 1)],
        send_sem=reply_send,
        recv_sem=reply_recv,
        device_id=0,
        device_id_type=LOGICAL,
    )
    answers.wait_send()
    answers.wait_recv()


def finish_kernel(mine, back, sums, potential, moments, sem):
    whole = pltpu.make_async_copy(sums, moments, sem)
    whole.start()
    batches = potential.shape[0]
    chosen = mine[...].astype(BF16)
    for h in range(2):
        high, rest = split(back[:, h, :])
        middle, low = split(rest)
        total = (
            dot(chosen, high.astype(BF16))
            + dot(chosen, middle.astype(BF16))
            + dot(chosen, low.astype(BF16))
        )
        potential[:, h * 128 : (h + 1) * 128] = total[:batches]
    whole.wait()


VMEM = pl.BlockSpec(memory_space=pltpu.VMEM)
HBM = pl.BlockSpec(memory_space=pltpu.HBM)
SMEM = pl.BlockSpec(memory_space=pltpu.SMEM)


def body(
    point_coords,
    charge,
    shell_index,
    neighbours,
    neighbour_count,
    batch_load,
    atom_coords,
    owner_slot,
):
    batches, points = charge.shape
    slots = neighbours.shape[1]
    devices = lax.axis_size("gx") * lax.axis_size("gy")
    owned = owner_slot.shape[0] // devices
    spaces = batches * slots
    sds = jax.ShapeDtypeStruct
    green_table = green_blocks()
    sums, mine, back = pl.pallas_call(
        fused_kernel,
        out_shape=(
            sds((owned, LM * SHELLS), F32),
            sds((8, devices), F32),
            sds((devices, 2, 128), F32),
        ),
        in_specs=[SMEM] + [HBM] * 9,
        out_specs=(VMEM, VMEM, VMEM),
        scratch_shapes=[
            pltpu.SMEM((batches, slots), jnp.int32),
            pltpu.SMEM((batches,), jnp.int32),
            pltpu.SMEM(owner_slot.shape, jnp.int32),
            pltpu.SMEM(atom_coords.shape, F32),
            pltpu.VMEM((3, batches, points), F32),
            pltpu.VMEM((batches, points), F32),
            pltpu.VMEM((batches, slots, points), jnp.int32),
            pltpu.VMEM(green_table.shape, BF16),
            pltpu.VMEM((4, devices), jnp.int32),
            pltpu.VMEM((4, spaces + 8, 128), F32),
            pltpu.VMEM((ROWS + 1, spaces + 8, 128), F32),
            pltpu.VMEM((devices + 1, PITCH, 128), F32),
            pltpu.VMEM((devices + 1, PITCH, 128), F32),
            pltpu.VMEM((2, (devices + 1) * KP, 128), F32),
            pltpu.VMEM((2, devices + 8, 128), F32),
            pltpu.VMEM((devices, SHELLS, 256), BF16),
            pltpu.VMEM(((HALF + 2) * SLOTP, 128), F32),
            pltpu.VMEM((LM * owned, 128), F32),
            pltpu.VMEM((LM * owned, 128), BF16),
            pltpu.VMEM(((KP + 1) * SLOTP, 128), F32),
            pltpu.VMEM((devices + 8, 2, 128), F32),
            pltpu.VMEM((devices, LANES), F32),
            pltpu.VMEM((devices, LANES), F32),
            pltpu.SemaphoreType.DMA((9,)),
            pltpu.SemaphoreType.DMA,
            pltpu.SemaphoreType.DMA((devices // WAVE,)),
            pltpu.SemaphoreType.DMA,
            pltpu.SemaphoreType.DMA,
            pltpu.SemaphoreType.DMA,
            pltpu.SemaphoreType.DMA,
        ],
        compiler_params=pltpu.CompilerParams(
            collective_id=0, has_side_effects=True, vmem_limit_bytes=34 << 20
        ),
        name="fused",
    )(
        batch_load,
        *[
            pltpu.with_memory_space_constraint(one, pltpu.HBM)
            for one in (
                neighbours,
                neighbour_count,
                owner_slot,
                atom_coords,
                jnp.transpose(point_coords, (1, 0, 2)),
                charge,
                shell_index,
                jnp.asarray(green_table),
                jnp.asarray(np.array(ORDER, dtype=np.int32).T),
            )
        ]
    )
    potential, moments = pl.pallas_call(
        finish_kernel,
        out_shape=(sds(charge.shape, F32), sds(sums.shape, F32)),
        in_specs=[VMEM] * 3,
        out_specs=(VMEM, HBM),
        scratch_shapes=[pltpu.SemaphoreType.DMA],
        compiler_params=pltpu.CompilerParams(vmem_limit_bytes=4 << 20),
        name="finish",
    )(mine, back, sums)
    return (potential, moments)


def solution(mesh):
    return jax.shard_map(
        body,
        mesh=mesh,
        in_specs=(
            P(("gx", "gy"), None, None),
            P(("gx", "gy"), None),
            P(("gx", "gy"), None, None),
            P(("gx", "gy"), None),
            P(("gx", "gy")),
            P(("gx", "gy")),
            P(),
            P(),
        ),
        out_specs=(P(("gx", "gy"), None), P(("gx", "gy"), None)),
        check_vma=False,
    )
```

```python
import math

import jax
import jax.numpy as jnp
import numpy as np
from jax import lax
from jax.experimental import pallas as pl
from jax.experimental.pallas import tpu as pltpu
from jax.sharding import PartitionSpec as P

LOGICAL = pl.DeviceIdType.LOGICAL
F32 = jnp.float32
BF16 = jnp.bfloat16
SHELLS = 64
LMAX = 6
LM = 49
KP = 56
HALF = 24
LANES = 8
SOFTEN = 0.01
ROWS = 10
PITCH = 16
SLOTP = 136
WAVE = 32


def green_blocks():
    rank = np.arange(SHELLS, dtype=np.float64)
    radius = 0.5 * np.exp(2.3 * rank / SHELLS)
    nearer = np.minimum(radius[:, None], radius[None, :])
    farther = np.maximum(radius[:, None], radius[None, :])
    full = np.stack(
        [
            4.0 * math.pi / (2 * d + 1) * nearer**d / farther ** (d + 1)
            for d in range(LMAX + 1)
        ]
    )
    full = np.concatenate([full, full], axis=2).astype(np.float32)
    high = full.astype(jnp.bfloat16)
    low = (full - high.astype(np.float32)).astype(jnp.bfloat16)
    upper = np.concatenate([high, low], axis=2)
    lower = np.concatenate([high, np.zeros_like(low)], axis=2)
    return np.concatenate([upper, lower], axis=1)


def split(x):
    high = x.astype(BF16).astype(F32)
    return high, x - high


def dot(a, b, dims=((1,), (0,))):
    return lax.dot_general(a, b, (dims, ((), ())), preferred_element_type=F32)


def harmonics(ux, uy, uz):
    cosine = [None]
    sine = [None]
    for m in range(1, LMAX + 1):
        if m == 1:
            cosine.append(ux)
            sine.append(uy)
        else:
            pc, ps = cosine[-1], sine[-1]
            cosine.append(pc * ux - ps * uy)
            sine.append(pc * uy + ps * ux)

    def norm(d, m):
        value = math.sqrt(
            (2 * d + 1) / (4 * math.pi) * math.factorial(d - m) / math.factorial(d + m)
        )
        return value * (math.sqrt(2.0) if m else 1.0)

    out = {}
    for m in range(LMAX + 1):
        start = norm(m, m) * float(math.prod(range(1, 2 * m, 2)))
        older, old = None, None
        for d in range(m, LMAX + 1):
            if d == m:
                now = start
            elif d == m + 1:
                now = uz * ((2 * m + 1) * start * norm(d, m) / norm(m, m))
            else:
                ca = (2 * d - 1) / (d - m) * norm(d, m) / norm(d - 1, m)
                cb = (d + m - 1) / (d - m) * norm(d, m) / norm(d - 2, m)
                now = (ca * uz) * old - cb * older
            if m == 0:
                out[d * d + d] = now if d else jnp.full(ux.shape, start, F32)
            else:
                out[d * d + d + m] = cosine[m] * now
                out[d * d + d - m] = sine[m] * now
            older, old = old, now
    return out


def visiting_order():
    every = [
        (dy, dz, dx, dc)
        for dy in range(4)
        for dz in range(4)
        for dx in range(4)
        for dc in range(2)
    ]

    def far(t):
        return sum(min(v, 4 - v) for v in t[:3])

    return every[:1] + sorted(every[1:], key=far, reverse=True)


ORDER = visiting_order()


def fused_kernel(
    *refs,
):
    load, given, refs = refs[0], refs[1:10], refs[10:]
    sums, mine, back = refs[:3]
    held, refs = refs[3:12], refs[12:]
    (
        place,
        src,
        pay,
        arrived,
        ys,
        ws,
        parts,
        acc,
        small,
        tables,
        reply,
        names,
        called,
        load_sem,
        send_sem,
        recv_sem,
        reply_send,
        reply_recv,
        name_send,
        name_recv,
    ) = refs
    labels, count, owner, atoms, coords, charge, shell, green, steps = held
    loads = [
        pltpu.make_async_copy(given[n], held[n], load_sem.at[n])
        for n in range(len(held))
    ]
    for one in loads:
        one.start()
    batches, slots = labels.shape
    spaces = batches * slots
    devices = pay.shape[0]
    owned = sums.shape[0]
    gy = lax.axis_index("gy")
    at = (lax.axis_index("gx"), gy // 8, lax.rem(gy, 8) // 2, lax.rem(gy, 2))
    spans, scales = (4, 4, 4, 2), (32, 8, 2, 1)
    moved_to = [
        [lax.rem(at[axis] + step, spans[axis]) * scales[axis] for step in range(spans[axis])]
        for axis in range(4)
    ]
    planes = {
        (dy, dz): moved_to[0][dy] + moved_to[1][dz] for dy in range(4) for dz in range(4)
    }
    lines = {
        (dx, dc): moved_to[2][dx] + moved_to[3][dc] for dx in range(4) for dc in range(2)
    }

    def peer(i, sign):
        dy, dz, dx, dc = [sign * d % span for d, span in zip(ORDER[i], spans)]
        return planes[dy, dz] + lines[dx, dc]

    barrier = pltpu.get_barrier_semaphore()
    for i in range(1, devices):
        pl.semaphore_signal(
            barrier, inc=1, device_id=peer(i, -1), device_id_type=LOGICAL
        )

    top = jnp.where(
        lax.broadcasted_iota(jnp.int32, (8, 128), 0) == 0,
        math.sqrt(1 / (4 * math.pi)),
        0.0,
    ).astype(F32)

    @pl.loop(0, devices)
    def _(i):
        for h in range(2):
            ys[h, pl.ds(pl.multiple_of(i * KP, 8), 8), :] = top
            ys[h, pl.ds(pl.multiple_of(i * KP + KP - 8, 8), 8), :] = jnp.zeros_like(top)

    for k in range(LM, KP):
        tables[k * SLOTP : k * SLOTP + devices, :] = jnp.zeros((devices, 128), F32)
    parts[(HALF * SLOTP) :, :] = jnp.zeros((SLOTP, 128), F32)

    for one in loads:
        one.wait()
    for b in range(batches):

        @pl.loop(0, slots, unroll=4)
        def _(s):
            label = labels[b, s]
            target = owner[label]
            row = b * slots + s
            for c in range(3):
                place[c, pl.ds(row, 1), :] = jnp.full((1, 128), atoms[c, label], F32)
            place[3, pl.ds(row, 1), :] = jnp.full(
                (1, 128), (target // owned).astype(F32), F32
            )
            src[10, pl.ds(row, 1), :] = jnp.full(
                (1, 128), lax.rem(target, owned).astype(F32), F32
            )

    slot_rank = lax.broadcasted_iota(jnp.int32, (slots, 128), 0)
    lane = lax.broadcasted_iota(jnp.int32, (slots, 128), 1)
    lives = []
    for b in range(batches):
        live = jnp.clip(load[0] - b, 0, 1).astype(F32)
        slot_live = jnp.clip(count[b] - slot_rank, 0, 1).astype(F32)
        here = slice(b * slots, (b + 1) * slots)
        lives.append(jnp.where(lane == b, slot_live * live, 0.0))
        for h in range(2):
            points = slice(h * 128, (h + 1) * 128)
            squared = 0.0
            for c in range(3):
                offset = coords[c, b : b + 1, points] - place[c, here, :]
                src[2 * c + h, here, :] = offset
                squared = squared + offset * offset
            closeness = slot_live / (1.0 + squared)
            total = jnp.sum(closeness, axis=0, keepdims=True)
            scaled = charge[b : b + 1, points] * live / total
            src[6 + h, here, :] = shell[b, :, points].astype(F32)
            src[8 + h, here, :] = slot_live * scaled

    row_of = 0
    for axis in range(4):
        there = lax.rem(steps[axis : axis + 1, :] + at[axis], spans[axis])
        row_of = row_of * spans[axis] + there
    goes = (place[3] == row_of.astype(F32)).astype(F32)
    goes = goes.T.astype(BF16)
    flat_pay = pay.reshape(devices * PITCH, 128)
    for r in range(ROWS + 1):
        high, rest = split(src[r])
        moved = dot(goes, high.astype(BF16))
        if r not in (6, 7, 10):
            middle, low = split(rest)
            moved = (
                moved + dot(goes, middle.astype(BF16)) + dot(goes, low.astype(BF16))
            )
        if r < ROWS:
            flat_pay[pl.ds(r, devices, stride=PITCH), :] = moved
        else:
            names[...] = moved[:, :LANES]
    lives = dot(goes, jnp.concatenate(lives, axis=0).astype(BF16))
    mine[...] = lives.T[:8]

    pl.semaphore_wait(barrier, devices - 1)

    def piece(ref, i, size=1):
        return ref.at[pl.ds(i, size), pl.ds(0, ROWS)]

    for i in range(1, devices):
        pltpu.make_async_remote_copy(
            src_ref=piece(pay, i),
            dst_ref=piece(arrived, i),
            send_sem=send_sem,
            recv_sem=recv_sem.at[i // WAVE],
            device_id=peer(i, 1),
            device_id_type=LOGICAL,
        ).start()

    def called_by(i, size):
        return names.at[pl.ds(i, size)], called.at[pl.ds(i, size)]

    for i in range(1, devices):
        here_name, there_name = called_by(i, 1)
        pltpu.make_async_remote_copy(
            src_ref=here_name,
            dst_ref=there_name,
            send_sem=name_send,
            recv_sem=name_recv,
            device_id=peer(i, 1),
            device_id_type=LOGICAL,
        ).start()
    called[0:1, :] = names[0:1, :]
    arrived[0] = pay[0]
    flat = arrived.reshape(devices * PITCH, 128)
    shell_rank = lax.broadcasted_iota(jnp.int32, (SHELLS, 128), 0).astype(F32)

    def shapes(g):
        for h in range(2):

            def row(r):
                return flat[pl.ds(g * 8 * PITCH + 2 * r + h, 8, stride=PITCH), :]

            dx, dy, dz = row(0), row(1), row(2)
            squared = dx * dx + dy * dy + dz * dz
            scale = lax.rsqrt(squared + SOFTEN)
            ws[h, pl.ds(pl.multiple_of(g * 8, 8), 8), :] = row(4) / (1.0 + squared)
            values = harmonics(dx * scale, dy * scale, dz * scale)
            for k in range(1, LM):
                ys[h, pl.ds(g * 8 * KP + k, 8, stride=KP), :] = values[k]

    def forward(i):
        stack, hot = [], []
        for h in range(2):
            y = ys[h, pl.ds(pl.multiple_of(i * KP, 8), KP), :]
            weighted = y * ws[h, pl.ds(i, 1), :]
            high, low = split(weighted)
            stack.append(jnp.concatenate([high, low], axis=0).astype(BF16))
            shells = flat[pl.ds(i * PITCH + 6 + h, 1), :]
            hot.append((shells == shell_rank).astype(F32).astype(BF16))
        hot = jnp.concatenate(hot, axis=1)
        both = dot(jnp.concatenate(stack, axis=1), hot, ((1,), (1,)))
        part = both[:KP] + both[KP:]
        parts[pl.ds(i, HALF, stride=SLOTP), :] = jnp.concatenate(
            [part[:HALF], part[HALF : 2 * HALF]], axis=1
        )
        parts[pl.ds(HALF * SLOTP + i, 1), :SHELLS] = part[2 * HALF : LM]

    def landed(g, size):
        pltpu.make_async_remote_copy(
            src_ref=piece(pay, 1, size),
            dst_ref=piece(arrived, 1, size),
            send_sem=send_sem,
            recv_sem=recv_sem.at[g],
            device_id=0,
            device_id_type=LOGICAL,
        ).wait_recv()

    @pl.loop(0, devices // WAVE)
    def _(g):
        @pl.when(g == 0)
        def _():
            landed(g, WAVE - 1)

        @pl.when(g > 0)
        def _():
            landed(g, WAVE)

        for q in range(WAVE // 8):
            shapes(g * (WAVE // 8) + q)

        for e in range(WAVE):
            forward(g * WAVE + e)

    here_names, there_names = called_by(1, devices - 1)
    called_all = pltpu.make_async_remote_copy(
        src_ref=here_names,
        dst_ref=there_names,
        send_sem=name_send,
        recv_sem=name_recv,
        device_id=0,
        device_id_type=LOGICAL,
    )
    called_all.wait_send()
    called_all.wait_recv()
    marks = jnp.broadcast_to(called[:, :1], (devices, 128))
    picks = (
        marks == lax.broadcasted_iota(jnp.int32, (devices, 128), 1).astype(F32)
    ).astype(F32)
    gather = picks[:, :owned].astype(BF16)
    combine = picks.T[:owned].astype(BF16)
    combine = jnp.concatenate([combine, combine], axis=1)
    left = lax.broadcasted_iota(jnp.int32, (owned, 128), 1) < SHELLS
    for k in range(HALF + 1):
        high, low = split(parts[k * SLOTP : k * SLOTP + devices, :])
        both = dot(combine, jnp.concatenate([high, low], axis=0).astype(BF16))
        other = pltpu.roll(both, SHELLS, 1)
        at_k = (k if k < HALF else LM - 1) * owned
        acc[at_k : at_k + owned, :] = jnp.where(left, both, other)
        if k < HALF:
            at_k += HALF * owned
            acc[at_k : at_k + owned, :] = jnp.where(left, other, both)

    for d in range(LMAX + 1):
        begin, end = d * d, (d + 1) * (d + 1)
        twice = acc[begin * owned : end * owned, :]
        high, low = split(twice)
        wide = lax.broadcasted_iota(jnp.int32, twice.shape, 1) < SHELLS
        both = dot(jnp.where(wide, high, low).astype(BF16), green[d])
        thigh, tlow = split(both[:, :128] + both[:, 128:])
        small[begin * owned : end * owned, :] = jnp.where(wide, thigh, tlow).astype(BF16)
    for k in range(0, LM, 2):
        many = min(2, LM - k)
        rows = [small[n * owned : (n + 1) * owned, :] for n in range(k, k + many)]
        picked = dot(gather, jnp.concatenate(rows, axis=1))
        for n in range(many):
            at_k = (k + n) * SLOTP
            tables[at_k : at_k + devices, :] = picked[:, n * 128 : (n + 1) * 128]

    def evaluate(i):
        table = tables[pl.ds(i, KP, stride=SLOTP), :].astype(BF16)
        hot = jnp.concatenate(
            [
                (flat[pl.ds(i * PITCH + 6 + h, 1), :] == shell_rank).astype(F32).astype(BF16)
                for h in range(2)
            ],
            axis=1,
        )
        picked = dot(table, jnp.concatenate([hot, hot], axis=0))
        for h in range(2):
            y = ys[h, pl.ds(pl.multiple_of(i * KP, 8), KP), :]
            total = jnp.sum(
                picked[:, h * 128 : (h + 1) * 128] * y, axis=0, keepdims=True
            )
            reply[i, h : h + 1, :] = total

    def answer(begin, end):
        for i in range(max(begin, 1), end):
            pltpu.make_async_remote_copy(
                src_ref=reply.at[i],
                dst_ref=back.at[i],
                send_sem=reply_send,
                recv_sem=reply_recv,
                device_id=peer(i, -1),
                device_id_type=LOGICAL,
            ).start()

    pairs = LM // 2
    for g in range(devices // WAVE):
        for i in range(g * WAVE, (g + 1) * WAVE):
            evaluate(i)
        for n in range(g * WAVE * pairs // devices, (g + 1) * WAVE * pairs // devices):
            first = acc[2 * n * owned : (2 * n + 1) * owned, :]
            second = acc[(2 * n + 1) * owned : (2 * n + 2) * owned, :]
            sums[:, n * 128 : (n + 1) * 128] = jnp.where(left, first, second)
        answer(g * WAVE, (g + 1) * WAVE)
    back[0] = reply[0]
    sums[:, pairs * 128 :] = acc[(LM - 1) * owned : LM * owned, :SHELLS]

    everything = pltpu.make_async_remote_copy(
        src_ref=piece(pay, 1, devices - 1),
        dst_ref=piece(arrived, 1, devices - 1),
        send_sem=send_sem,
        recv_sem=recv_sem.at[0],
        device_id=0,
        device_id_type=LOGICAL,
    )
    everything.wait_send()
    answers = pltpu.make_async_remote_copy(
        src_ref=reply.at[pl.ds(1, devices - 1)],
        dst_ref=back.at[pl.ds(1, devices - 1)],
        send_sem=reply_send,
        recv_sem=reply_recv,
        device_id=0,
        device_id_type=LOGICAL,
    )
    answers.wait_send()
    answers.wait_recv()


def finish_kernel(mine, back, sums, potential, moments, sem):
    whole = pltpu.make_async_copy(sums, moments, sem)
    whole.start()
    batches = potential.shape[0]
    chosen = mine[...].astype(BF16)
    for h in range(2):
        high, rest = split(back[:, h, :])
        middle, low = split(rest)
        total = (
            dot(chosen, high.astype(BF16))
            + dot(chosen, middle.astype(BF16))
            + dot(chosen, low.astype(BF16))
        )
        potential[:, h * 128 : (h + 1) * 128] = total[:batches]
    whole.wait()


VMEM = pl.BlockSpec(memory_space=pltpu.VMEM)
HBM = pl.BlockSpec(memory_space=pltpu.HBM)
SMEM = pl.BlockSpec(memory_space=pltpu.SMEM)


def body(
    point_coords,
    charge,
    shell_index,
    neighbours,
    neighbour_count,
    batch_load,
    atom_coords,
    owner_slot,
):
    batches, points = charge.shape
    slots = neighbours.shape[1]
    devices = lax.axis_size("gx") * lax.axis_size("gy")
    owned = owner_slot.shape[0] // devices
    spaces = batches * slots
    sds = jax.ShapeDtypeStruct
    green_table = green_blocks()
    sums, mine, back = pl.pallas_call(
        fused_kernel,
        out_shape=(
            sds((owned, LM * SHELLS), F32),
            sds((8, devices), F32),
            sds((devices, 2, 128), F32),
        ),
        in_specs=[SMEM] + [HBM] * 9,
        out_specs=(VMEM, VMEM, VMEM),
        scratch_shapes=[
            pltpu.SMEM((batches, slots), jnp.int32),
            pltpu.SMEM((batches,), jnp.int32),
            pltpu.SMEM(owner_slot.shape, jnp.int32),
            pltpu.SMEM(atom_coords.shape, F32),
            pltpu.VMEM((3, batches, points), F32),
            pltpu.VMEM((batches, points), F32),
            pltpu.VMEM((batches, slots, points), jnp.int32),
            pltpu.VMEM(green_table.shape, BF16),
            pltpu.VMEM((4, devices), jnp.int32),
            pltpu.VMEM((4, spaces, 128), F32),
            pltpu.VMEM((ROWS + 1, spaces, 128), F32),
            pltpu.VMEM((devices, PITCH, 128), F32),
            pltpu.VMEM((devices, PITCH, 128), F32),
            pltpu.VMEM((2, devices * KP, 128), F32),
            pltpu.VMEM((2, devices, 128), F32),
            pltpu.VMEM(((HALF + 1) * SLOTP, 128), F32),
            pltpu.VMEM((LM * owned, 128), F32),
            pltpu.VMEM((LM * owned, 128), BF16),
            pltpu.VMEM((KP * SLOTP, 128), F32),
            pltpu.VMEM((devices, 2, 128), F32),
            pltpu.VMEM((devices, LANES), F32),
            pltpu.VMEM((devices, LANES), F32),
            pltpu.SemaphoreType.DMA((9,)),
            pltpu.SemaphoreType.DMA,
            pltpu.SemaphoreType.DMA((devices // WAVE,)),
            pltpu.SemaphoreType.DMA,
            pltpu.SemaphoreType.DMA,
            pltpu.SemaphoreType.DMA,
            pltpu.SemaphoreType.DMA,
        ],
        compiler_params=pltpu.CompilerParams(
            collective_id=0, has_side_effects=True, vmem_limit_bytes=34 << 20
        ),
        name="fused",
    )(
        batch_load,
        *[
            pltpu.with_memory_space_constraint(one, pltpu.HBM)
            for one in (
                neighbours,
                neighbour_count,
                owner_slot,
                atom_coords,
                jnp.transpose(point_coords, (1, 0, 2)),
                charge,
                shell_index,
                jnp.asarray(green_table),
                jnp.asarray(np.array(ORDER, dtype=np.int32).T),
            )
        ]
    )
    potential, moments = pl.pallas_call(
        finish_kernel,
        out_shape=(sds(charge.shape, F32), sds(sums.shape, F32)),
        in_specs=[VMEM] * 3,
        out_specs=(VMEM, HBM),
        scratch_shapes=[pltpu.SemaphoreType.DMA],
        compiler_params=pltpu.CompilerParams(vmem_limit_bytes=4 << 20),
        name="finish",
    )(mine, back, sums)
    return (potential, moments)


def solution(mesh):
    return jax.shard_map(
        body,
        mesh=mesh,
        in_specs=(
            P(("gx", "gy"), None, None),
            P(("gx", "gy"), None),
            P(("gx", "gy"), None, None),
            P(("gx", "gy"), None),
            P(("gx", "gy")),
            P(("gx", "gy")),
            P(),
            P(),
        ),
        out_specs=(P(("gx", "gy"), None), P(("gx", "gy"), None)),
        check_vma=False,
    )
```
